512 devices in a mesh: dp: 64 (over z, x), head: 8 (over y, core).
Axes of the slice: x: 4, y: 4, z: 16, core: 2. Of those that a mesh axis runs over, the one named last changes fastest.
Arguments:
- queries: bfloat16 [16384, 8192], P('dp', 'head'), may hold values from -6 to 6
- keys: bfloat16 [16384, 1024], P('dp', 'head'), may hold values from -6 to 6
- values: bfloat16 [16384, 1024], P('dp', 'head'), may hold values from -6 to 6
- output_grad: bfloat16 [16384, 4096], P('dp', 'head'), may hold values from -6 to 6
- out_weight: bfloat16 [8192, 4096], P(('head', 'dp')), may hold values from -0.0625 to 0.0625
- lengths: int32 [64], replicated, may hold values from 1 to 512, 16384 in all
Outputs:
- layer_out: bfloat16 [16384, 4096], P('dp', 'head')
- query_grad: bfloat16 [16384, 8192], P('dp', 'head')
- key_grad: bfloat16 [16384, 1024], P('dp', 'head')
- value_grad: bfloat16 [16384, 1024], P('dp', 'head')
The draws below stay inside these ranges and needn't reach their ends.
Inputs may be any that keep to these rules, and one draw needn't show every extreme that they name: Each of the 64 lengths is at least 1 and at most 512, they sum to 16384, and one equals 512.
All inputs are finite; a program needn't handle non-finite values.
Results may differ from the reference program's by a relative error of at most 0.028.
Values may be sent and summed in bfloat16 or wider, within the bound.
No kernel may reach another device: no remote copies, remote signals or barrier semaphores. Data moves between devices by JAX's collectives and lax.ppermute only.
A program may use at most 128 MiB of HBM per device.

```python
import math
import jax
import jax.numpy as jnp
import numpy as np
from jax import lax

HEADS = 64
KV_HEADS = 8
HD = 128
DW = 4096
TOK_DEV = 256
SPAN = 2
LENGTH = 16384
MOST = 512
DOCS = 64
N_DP = 64


def draw_queries(key, part):
    base = jnp.clip(jax.random.normal(jax.random.fold_in(key, 1), (LENGTH, HEADS * HD)), -4.0, 4.0)
    return base.astype(jnp.bfloat16)


def draw_keys(key, part):
    base = jnp.clip(jax.random.normal(jax.random.fold_in(key, 2), (LENGTH, KV_HEADS * HD)), -4.0, 4.0)
    return base.astype(jnp.bfloat16)


def block_levels(key, shape, pieces, low, top_value):
    factor_of = 1.0
    for position, blocks in pieces:
        steps = jax.random.uniform(jax.random.fold_in(jax.random.fold_in(key, 6), position), (blocks,), jnp.float32, low / len(pieces), top_value / len(pieces))
        factor_of = factor_of * jnp.repeat(jnp.exp(steps), shape[position] // blocks).reshape((-1,) + (1,) * (len(shape) - 1 - position))
    return factor_of


def split_up(count, total, limit, lean):
    loads = [(1 << 20) // math.isqrt(grade ** lean) + 1 for grade in range(2, count + 1)]
    surplus, holding = total - limit - (count - 1), [1] * (count - 1)
    while surplus > 0:
        candidates = [i for i in range(count - 1) if holding[i] < limit]
        whole, remaining = sum([loads[i] for i in candidates]), surplus
        for i in candidates:
            more = min(limit - holding[i], max(1, remaining * loads[i] // whole), surplus)
            holding[i] = holding[i] + more
            surplus = surplus - more
    return np.array([limit] + holding)


def ragged_sizes(key, number_of, total, limit, skew):
    if number_of == 2:
        one = jax.random.randint(key, (), max(1, total - limit), min(limit, total - 1) + 1)
        return jnp.stack([one, total - one])
    tallies = jnp.asarray(split_up(number_of, total, limit, skew), jnp.int32)
    twos = (number_of - 1) // 2
    giver, receiver = tallies[1:1 + 2 * twos:2], tallies[2:2 + 2 * twos:2]
    margin = jnp.minimum(giver - 1, limit - receiver)
    moved = jax.random.randint(jax.random.fold_in(key, 1), (twos,), 0, 1 << 20) % (margin + 1)
    tallies = tallies.at[1:1 + 2 * twos:2].set(giver - moved).at[2:2 + 2 * twos:2].set(receiver + moved)
    return tallies[jax.random.permutation(jax.random.fold_in(key, 2), number_of)]


def normal_values(key, extent, width, most, shards=(), held_as=jnp.bfloat16):
    array = jax.random.normal(key, extent, jnp.float32) * width
    if len(shards) > 0:
        array = block_levels(key, extent, shards, -0.22, 0.18) * array
    return jnp.clip(array, min=-most, max=most).astype(held_as)


def setup_inputs(seed: int = 0) -> dict:
    splits = jax.random.split(jax.random.key(seed), 7)
    queries = draw_queries(jax.random.fold_in(splits[6], 71), 0)
    keys = draw_keys(jax.random.fold_in(splits[6], 71), 0)
    values = normal_values(splits[2], (LENGTH, KV_HEADS * HD), 1.0, 6.0, ((0, 64), (1, 8)))
    output_grad = normal_values(splits[3], (LENGTH, DW), 1.0, 6.0, ((0, 64), (1, 8)))
    out_weight = normal_values(splits[4], (HEADS * HD, DW), (HEADS * HD) ** -0.5, 0.0625, ((0, 512),))
    lengths = ragged_sizes(splits[5], DOCS, LENGTH, MOST, 2).astype(jnp.int32)
    return {"queries": queries, "keys": keys, "values": values, "output_grad": output_grad, "out_weight": out_weight, "lengths": lengths}


masked_score = -1e+30

def doc_start(lengths, positions):
    lengths = lengths.astype(jnp.int32)
    doc_ends = jnp.cumsum(lengths).astype(jnp.int32)
    closed = doc_ends[None, :] <= positions[:, None]
    return lax.optimization_barrier(jnp.sum(jnp.where(closed, lengths[None, :], 0), axis=1)).astype(jnp.int32)

def attend(queries, key_rows, value_rows, d_attended, visible, head_dim):
    row_count = queries.shape[0]
    kv_heads = key_rows.shape[1] // head_dim
    group_ratio = queries.shape[1] // key_rows.shape[1]
    scaling = 1.0 / math.sqrt(head_dim)
    grouped = queries.reshape(row_count, kv_heads, group_ratio, head_dim).astype(jnp.float32)
    keyed = key_rows.reshape(-1, kv_heads, head_dim).astype(jnp.float32)
    valued = value_rows.reshape(-1, kv_heads, head_dim).astype(jnp.float32)
    upstream = d_attended.reshape(row_count, kv_heads, group_ratio, head_dim).astype(jnp.float32)
    scores = jnp.einsum('tgrd,ngd->grtn', grouped, keyed) * scaling
    scores = jnp.where(visible[None, None], scores, masked_score)
    maximum = lax.optimization_barrier(jnp.max(scores, axis=-1, keepdims=True))
    weights = jnp.exp(scores - maximum)
    shares = weights / lax.optimization_barrier(jnp.sum(weights, axis=-1, keepdims=True))
    shares_low = lax.optimization_barrier(shares.astype(jnp.bfloat16)).astype(jnp.float32)
    attended = lax.optimization_barrier(jnp.einsum('grtn,ngd->tgrd', shares_low, valued).astype(jnp.bfloat16))
    attended_wide = attended.astype(jnp.float32)
    row_dots = lax.optimization_barrier(jnp.sum(upstream * attended_wide, axis=-1))
    d_shares = jnp.einsum('tgrd,ngd->grtn', upstream, valued)
    dscore = shares * (d_shares - jnp.transpose(row_dots, (1, 2, 0))[..., None]) * scaling
    dscore = lax.optimization_barrier(dscore.astype(jnp.bfloat16)).astype(jnp.float32)
    query_grad = jnp.einsum('grtn,ngd->tgrd', dscore, keyed).astype(jnp.bfloat16)
    key_part = jnp.einsum('grtn,tgrd->ngd', dscore, grouped)
    value_part = jnp.einsum('grtn,tgrd->ngd', shares_low, upstream)
    return (attended.reshape(row_count, -1), query_grad.reshape(row_count, -1), key_part.reshape(-1, kv_heads * head_dim), value_part.reshape(-1, kv_heads * head_dim))

def reference(queries, keys, values, output_grad, out_weight, lengths):
    block_rows = TOK_DEV
    window_rows = (SPAN + 1) * block_rows
    padding = SPAN * block_rows
    kv_width = keys.shape[1]
    d_attended = jnp.dot(output_grad, out_weight.T, preferred_element_type=jnp.float32).astype(jnp.bfloat16)
    padded_keys = jnp.concatenate([jnp.zeros((padding, kv_width), keys.dtype), keys], axis=0)
    padded_values = jnp.concatenate([jnp.zeros((padding, kv_width), values.dtype), values], axis=0)

    def one_block(running, block_index):
        key_acc, value_acc = running
        first_row = (block_index * block_rows).astype(jnp.int32)
        query_block = lax.dynamic_slice_in_dim(queries, first_row, block_rows, 0)
        grad_block = lax.dynamic_slice_in_dim(d_attended, first_row, block_rows, 0)
        key_block = lax.dynamic_slice_in_dim(padded_keys, first_row, window_rows, 0)
        value_block = lax.dynamic_slice_in_dim(padded_values, first_row, window_rows, 0)
        positions = first_row + jnp.arange(block_rows, dtype=jnp.int32)
        starts = doc_start(lengths, positions)
        key_positions = first_row - padding + jnp.arange(window_rows, dtype=jnp.int32)
        visible = (key_positions[None, :] >= starts[:, None]) & (key_positions[None, :] <= positions[:, None])
        attended, query_grad, key_part, value_part = attend(query_block, key_block, value_block, grad_block, visible, HD)
        key_acc = lax.dynamic_update_slice_in_dim(key_acc, lax.dynamic_slice_in_dim(key_acc, first_row, window_rows, 0) + key_part, first_row, 0)
        value_acc = lax.dynamic_update_slice_in_dim(value_acc, lax.dynamic_slice_in_dim(value_acc, first_row, window_rows, 0) + value_part, first_row, 0)
        return ((key_acc, value_acc), (attended, query_grad))
    zeroed = jnp.zeros((N_DP * block_rows + padding, kv_width), jnp.float32)
    (key_acc, value_acc), (attended_blocks, query_blocks) = lax.scan(one_block, (zeroed, zeroed), jnp.arange(N_DP, dtype=jnp.int32))
    attended_all = attended_blocks.reshape(-1, attended_blocks.shape[-1])
    layer_out = jnp.dot(attended_all, out_weight, preferred_element_type=jnp.float32).astype(jnp.bfloat16)
    query_grad = query_blocks.reshape(-1, query_blocks.shape[-1])
    return (layer_out, query_grad, key_acc[padding:].astype(jnp.bfloat16), value_acc[padding:].astype(jnp.bfloat16))
```

```python
import math

import jax
import jax.numpy as jnp
from jax import lax
from jax.sharding import Mesh
from jax.sharding import PartitionSpec as P

HD = 128
SPAN = 2
DP = ("dp_0", "dp_1")
HEAD_DP = ("head", "dp_0", "dp_1")


masked_score = -1e30


def gather_axes(x, axes, dim):
    filled = x
    for number in range(len(axes) - 1, -1, -1):
        filled = lax.all_gather(filled, axes[number], axis=dim, tiled=True)
    return filled


def in_order(pieces, dim):
    pieces = jnp.moveaxis(pieces, 0, dim)
    shape = pieces.shape
    return pieces.reshape(*shape[:dim], shape[dim] * shape[dim + 1], *shape[dim + 2 :])


def from_everyone(x, axis):
    size = lax.axis_size(axis)
    return lax.all_to_all(jnp.broadcast_to(x[None], (size, *x.shape)), axis, 0, 0, tiled=True)


def gather_directly(x, axis, dim):
    return in_order(from_everyone(x, axis), dim)


def passed_along(block, axis, distance):
    devices = range(lax.axis_size(axis))
    route = [(i - distance, i) for i in devices if i - distance in devices]
    return lax.ppermute(block, axis, route)


def in_blocks(x, dim, size):
    before, after = (x.shape[:dim], x.shape[dim + 1 :])
    return jnp.moveaxis(x.reshape(*before, size, -1, *after), dim, 0)


def sent_and_summed(x, axis, dim):
    pieces = in_blocks(x, dim, lax.axis_size(axis))
    arrived = lax.all_to_all(pieces, axis, split_axis=0, concat_axis=0, tiled=True)
    return arrived.astype(jnp.float32).sum(axis=0)


def doc_start(lengths, positions):
    doc_ends = jnp.cumsum(lengths)
    closed = doc_ends[None, :] <= positions[:, None]
    return jnp.sum(jnp.where(closed, lengths[None, :], 0), axis=1)


def attend(queries, key_rows, value_rows, d_attended, visible, head_dim):
    row_count = queries.shape[0]
    kv_heads = key_rows.shape[1] // head_dim
    group_ratio = queries.shape[1] // key_rows.shape[1]
    scaling = 1.0 / math.sqrt(head_dim)
    grouped = queries.reshape(row_count, kv_heads, group_ratio, head_dim)
    keyed = key_rows.reshape(-1, kv_heads, head_dim)
    valued = value_rows.reshape(-1, kv_heads, head_dim)
    upstream = d_attended.reshape(row_count, kv_heads, group_ratio, head_dim)
    scores = (
        jnp.einsum("tgrd,ngd->grtn", grouped, keyed, preferred_element_type=jnp.float32) * scaling
    )
    scores = jnp.where(visible[None, None], scores, masked_score)
    maximum = jnp.max(scores, axis=-1, keepdims=True)
    weights = jnp.exp(scores - maximum)
    shares = weights / jnp.sum(weights, axis=-1, keepdims=True)
    shares_low = shares.astype(jnp.bfloat16)
    attended = jnp.einsum(
        "grtn,ngd->tgrd", shares_low, valued, preferred_element_type=jnp.float32
    ).astype(jnp.bfloat16)
    row_dots = jnp.sum(upstream.astype(jnp.float32) * attended.astype(jnp.float32), axis=-1)
    d_shares = jnp.einsum("tgrd,ngd->grtn", upstream, valued, preferred_element_type=jnp.float32)
    dscore = (shares * (d_shares - jnp.transpose(row_dots, (1, 2, 0))[..., None]) * scaling).astype(
        jnp.bfloat16
    )
    query_grad = jnp.einsum(
        "grtn,ngd->tgrd", dscore, keyed, preferred_element_type=jnp.float32
    ).astype(jnp.bfloat16)
    key_part = jnp.einsum("grtn,tgrd->ngd", dscore, grouped, preferred_element_type=jnp.float32)
    value_part = jnp.einsum(
        "grtn,tgrd->ngd", shares_low, upstream, preferred_element_type=jnp.float32
    )
    return (
        attended.reshape(row_count, -1),
        query_grad.reshape(row_count, -1),
        key_part.reshape(-1, kv_heads * head_dim),
        value_part.reshape(-1, kv_heads * head_dim),
    )


def on_device(queries, keys, values, output_grad, out_weight, lengths):
    block_rows = queries.shape[0]
    device = lax.axis_index(DP)
    group_weight = lax.all_gather(out_weight, DP, axis=0, tiled=True)
    upstream_all = gather_directly(output_grad, "head", 1)
    d_attended = jnp.einsum(
        "tc,rc->tr", upstream_all, group_weight, preferred_element_type=jnp.float32
    ).astype(jnp.bfloat16)
    earlier = [passed_along((keys, values), DP, offset) for offset in range(1, SPAN + 1)]
    key_rows = jnp.concatenate([couple[0] for couple in earlier[::-1]] + [keys], axis=0)
    value_rows = jnp.concatenate([couple[1] for couple in earlier[::-1]] + [values], axis=0)
    owner_positions = device * block_rows + jnp.arange(block_rows, dtype=jnp.int32)
    owner_starts = doc_start(lengths, owner_positions)
    key_positions = (device - SPAN) * block_rows + jnp.arange(
        (SPAN + 1) * block_rows, dtype=jnp.int32
    )
    visible = (key_positions[None, :] >= owner_starts[:, None]) & (
        key_positions[None, :] <= owner_positions[:, None]
    )
    first_row = 0 * block_rows
    attended, query_grad, key_part, value_part = attend(
        queries, key_rows, value_rows, d_attended, visible, HD
    )
    padding = jnp.zeros((first_row, key_part.shape[1]), jnp.float32)
    attended, query_grad, key_all, value_all = (
        attended,
        query_grad,
        jnp.concatenate([padding, key_part], axis=0),
        jnp.concatenate([padding, value_part], axis=0),
    )
    projected = jnp.dot(attended, group_weight, preferred_element_type=jnp.float32)
    layer_out = sent_and_summed(projected.astype(jnp.bfloat16), "head", 1).astype(jnp.bfloat16)

    def block_of(all_rows, offset):
        return all_rows[(SPAN - offset) * block_rows : (SPAN - offset + 1) * block_rows]

    key_home = block_of(key_all, 0)
    value_home = block_of(value_all, 0)
    for offset in range(1, SPAN + 1):
        returned = (
            passed_along(block_of(key_all, offset).astype(jnp.bfloat16), DP, -offset).astype(
                jnp.float32
            ),
            passed_along(block_of(value_all, offset).astype(jnp.bfloat16), DP, -offset).astype(
                jnp.float32
            ),
        )
        key_home = key_home + returned[0]
        value_home = value_home + returned[1]
    return (layer_out, query_grad, key_home.astype(jnp.bfloat16), value_home.astype(jnp.bfloat16))


def solution(mesh):
    finer = Mesh(mesh.devices.reshape(16, 4, mesh.shape["head"]), ("dp_0", "dp_1", "head"))
    placed = (P(DP, "head"), P(DP, "head"), P(DP, "head"), P(DP, "head"), P(HEAD_DP, None), P())
    return jax.shard_map(
        on_device,
        mesh=finer,
        in_specs=placed,
        out_specs=(P(DP, "head"), P(DP, "head"), P(DP, "head"), P(DP, "head")),
        check_vma=False,
    )
```

```python
import functools
import math

import jax
import jax.numpy as jnp
from jax import lax
from jax.experimental import pallas as pl
from jax.experimental.pallas import tpu as pltpu
from jax.sharding import Mesh
from jax.sharding import PartitionSpec as P

HD=128
LOG2E=1.4426950408889634
NT=(((1,),(1,)),((),()))

def dot_nt(a,b):
    return lax.dot_general(a,b,NT,preferred_element_type=jnp.float32)
def dot_nn(a,b):
    return jnp.dot(a,b,preferred_element_type=jnp.float32)

def forward_body(scaling, group, lengths, place, q, k2, k1, k0, v2, v1, v0, att, shares, bias, vt):
    rows = q.shape[0]
    blocks = 3
    @pl.when(pl.program_id(0) == 0)
    def _():
        first = place[0] * rows
        at = first + lax.broadcasted_iota(jnp.int32, (1, rows), 1)
        def doc(d, carry):
            end, start = carry
            end = end + lengths[d]
            return end, jnp.where(end <= at, end, start)
        _, start = lax.fori_loop(0, lengths.shape[0], doc, (jnp.int32(0), jnp.zeros((1, rows), jnp.int32)))
        keyed = first - (blocks - 1) * rows + lax.broadcasted_iota(jnp.int32, (blocks * rows, rows), 0)
        bias[...] = jnp.where((keyed >= start) & (keyed <= at), 0.0, -1e30)
        for j, v in enumerate((v2, v1, v0)):
            vt[:, j * rows:(j + 1) * rows] = v[...].T
    for h in range(group):
        cols = slice(h * HD, (h + 1) * HD)
        qh = q[:, cols]
        s = [dot_nt(k[...], qh) * (scaling * LOG2E) + bias[j * rows:(j + 1) * rows, :] for j, k in enumerate((k2, k1, k0))]
        top = functools.reduce(jnp.maximum, [jnp.max(x, axis=0, keepdims=True) for x in s])
        e = [jnp.exp2(x - top) for x in s]
        inv = 1.0 / sum(jnp.sum(x, axis=0, keepdims=True) for x in e)
        out = jnp.zeros((HD, rows), jnp.float32)
        for j, x in enumerate(e):
            p = (x * inv).astype(jnp.bfloat16)
            shares[h, j * rows:(j + 1) * rows, :] = p
            out = out + dot_nn(vt[:, j * rows:(j + 1) * rows], p)
        att[:, cols] = out.T.astype(jnp.bfloat16)

def forward(lengths, place, q, ks, vs, group=2):
    rows, width = q.shape
    heads = width // HD
    whole = pl.BlockSpec((rows, HD), lambda i: (0, 0))
    smem = pl.BlockSpec(memory_space=pltpu.SMEM)
    return pl.pallas_call(
        functools.partial(forward_body, 1.0 / math.sqrt(HD), group),
        grid=(heads // group,),
        in_specs=[smem, smem, pl.BlockSpec((rows, group * HD), lambda i: (0, i))] + [whole] * 6,
        out_specs=[pl.BlockSpec((rows, group * HD), lambda i: (0, i)),
                   pl.BlockSpec((group, 3 * rows, rows), lambda i: (i, 0, 0))],
        out_shape=[jax.ShapeDtypeStruct((rows, width), jnp.bfloat16),
                   jax.ShapeDtypeStruct((heads, 3 * rows, rows), jnp.bfloat16)],
        scratch_shapes=[pltpu.VMEM((3 * rows, rows), jnp.float32), pltpu.VMEM((HD, 3 * rows), jnp.bfloat16)],
        compiler_params=pltpu.CompilerParams(dimension_semantics=("arbitrary",)),
        name="attend_forward",
    )(lengths, place, q, *ks, *vs)

def backward_body(scaling, group, parts, *refs):
    (q, k2, k1, k0, v2, v1, v0, da_parts, att, shares, dq, dk2, dk1, dk0, dv2, dv1, dv0, kt, dka, dva) = refs
    rows = q.shape[0]
    step = pl.program_id(0)
    @pl.when(step == 0)
    def _():
        for j, k in enumerate((k2, k1, k0)):
            kt[:, j * rows:(j + 1) * rows] = k[...].T
        dka[...] = jnp.zeros_like(dka)
        dva[...] = jnp.zeros_like(dva)
    for h in range(group):
        cols = slice(h * HD, (h + 1) * HD)
        qh = q[:, cols]
        da = sum(da_parts[i, :, cols].astype(jnp.float32) for i in range(parts)).astype(jnp.bfloat16)
        prod = da.astype(jnp.float32) * att[:, cols].astype(jnp.float32)
        dots = jnp.sum(prod.T, axis=0, keepdims=True)
        out = jnp.zeros((HD, rows), jnp.float32)
        for j, v in enumerate((v2, v1, v0)):
            own = slice(j * rows, (j + 1) * rows)
            p = shares[h, own, :]
            d = dot_nt(v[...], da)
            ds = (p.astype(jnp.float32) * (d - dots)).astype(jnp.bfloat16)
            out = out + dot_nn(kt[:, own], ds)
            dka[own, :] += dot_nn(ds, qh)
            dva[own, :] += dot_nn(p, da)
        dq[:, cols] = (out.T * scaling).astype(jnp.bfloat16)
    @pl.when(step == pl.num_programs(0) - 1)
    def _():
        for j, (dk, dv) in enumerate(((dk2, dv2), (dk1, dv1), (dk0, dv0))):
            own = slice(j * rows, (j + 1) * rows)
            dk[...] = (dka[own, :] * scaling).astype(dk.dtype)
            dv[...] = dva[own, :].astype(dv.dtype)

def backward(q, ks, vs, da_parts, att, shares, group=2):
    rows, width = q.shape
    heads = width // HD
    parts = da_parts.shape[0]
    whole = pl.BlockSpec((rows, HD), lambda i: (0, 0))
    head = pl.BlockSpec((rows, group * HD), lambda i: (0, i))
    piece = lambda t: jax.ShapeDtypeStruct((rows, HD), t)
    bf, f32 = jnp.bfloat16, jnp.float32
    return pl.pallas_call(
        functools.partial(backward_body, 1.0 / math.sqrt(HD), group, parts),
        grid=(heads // group,),
        in_specs=[head] + [whole] * 6 + [pl.BlockSpec((parts, rows, group * HD), lambda i: (0, 0, i)), head,
                  pl.BlockSpec((group, 3 * rows, rows), lambda i: (i, 0, 0))],
        out_specs=[head] + [whole] * 6,
        out_shape=[jax.ShapeDtypeStruct((rows, width), bf)] + [piece(bf), piece(bf), piece(f32)] * 2,
        scratch_shapes=[pltpu.VMEM((HD, 3 * rows), bf), pltpu.VMEM((3 * rows, HD), f32), pltpu.VMEM((3 * rows, HD), f32)],
        compiler_params=pltpu.CompilerParams(dimension_semantics=("arbitrary",)),
        name="attend_backward",
    )(q, *ks, *vs, da_parts, att, shares)

def back_body(og, w, out, lhs):
    @pl.when(pl.program_id(0) == 0)
    def _():
        for h in range(og.shape[0]):
            lhs[:, h * HD:(h + 1) * HD] = og[h]
    out[...] = dot_nt(lhs[...], w[...]).astype(out.dtype)


def project_back(og, w, block=256):
    heads, tokens, _ = og.shape
    rows, columns = w.shape
    return pl.pallas_call(
        back_body,
        grid=(rows // block,),
        in_specs=[pl.BlockSpec((heads, tokens, HD), lambda i: (0, 0, 0)), pl.BlockSpec((block, columns), lambda i: (i, 0))],
        out_specs=pl.BlockSpec((tokens, block), lambda i: (0, i)),
        out_shape=jax.ShapeDtypeStruct((tokens, rows), jnp.bfloat16),
        scratch_shapes=[pltpu.VMEM((tokens, columns), jnp.bfloat16)],
        compiler_params=pltpu.CompilerParams(dimension_semantics=("arbitrary",)),
        name="project_back",
    )(og, w)


def out_body(att, w, out):
    done = dot_nn(att[...], w[...]).astype(out.dtype)
    for h in range(out.shape[0]):
        out[h] = done[:, h * HD:(h + 1) * HD]


def project_out(att, w, block=256):
    tokens, rows = att.shape
    columns = w.shape[1]
    return pl.pallas_call(
        out_body,
        grid=(columns // block,),
        in_specs=[pl.BlockSpec((tokens, rows), lambda i: (0, 0)), pl.BlockSpec((rows, block), lambda i: (0, i))],
        out_specs=pl.BlockSpec((block // HD, tokens, HD), lambda i: (i, 0, 0)),
        out_shape=jax.ShapeDtypeStruct((columns // HD, tokens, HD), jnp.bfloat16),
        compiler_params=pltpu.CompilerParams(dimension_semantics=("arbitrary",)),
        name="project_out",
    )(att, w)

X = "x"
HEAD = ("y", "core")
DP = ("z", "x")


def swap(pieces, axis):
    return lax.all_to_all(pieces, axis, 0, 0, tiled=True)


def everywhere(x, axis):
    return swap(jnp.broadcast_to(x[None], (lax.axis_size(axis), *x.shape)), axis)


def shifted(block, distance):
    size = lax.axis_size(DP)
    return lax.ppermute(block, DP, [(i, i + distance) for i in range(size) if 0 <= i + distance < size])


def on_device(queries, keys, values, output_grad, out_weight, lengths):
    rows = queries.shape[0]
    parts = lax.axis_size(X)
    heads = lax.axis_size(HEAD)
    place = lax.axis_index(DP).astype(jnp.int32).reshape(1)
    own_w = out_weight.reshape(out_weight.shape[0], heads, parts, HD).transpose(2, 0, 1, 3)
    own_w = swap(own_w.reshape(parts, out_weight.shape[0], heads * HD), X)
    weight = lax.all_gather(own_w.reshape(-1, heads * HD), "z", axis=0, tiled=True)
    pair = jnp.concatenate([keys, values], axis=1)
    earlier = [shifted(pair, offset) for offset in (2, 1)]
    grads = swap(output_grad.reshape(rows, parts, HD).transpose(1, 0, 2), X).reshape(parts * rows, HD)
    grads = everywhere(grads, HEAD)
    ks = [e[:, :HD] for e in earlier] + [keys]
    vs = [e[:, HD:] for e in earlier] + [values]
    attended, shares = forward(lengths, place, queries, ks, vs)
    attended_all = everywhere(attended, X).reshape(parts * rows, -1)
    d_parts = project_back(grads, weight).reshape(parts, rows, -1)
    d_parts = swap(d_parts, X)
    projected = swap(project_out(attended_all, weight), HEAD)
    projected = projected.astype(jnp.float32).sum(axis=0).astype(jnp.bfloat16)
    layer_out = swap(projected.reshape(parts, rows, HD), X).transpose(1, 0, 2).reshape(rows, parts * HD)
    query_grad, *returned = backward(queries, ks, vs, d_parts, attended, shares)
    k2, k1, k0, v2, v1, v0 = returned
    two = shifted(jnp.concatenate([k2, v2], axis=1), -2).astype(jnp.float32)
    one = shifted(jnp.concatenate([k1, v1], axis=1), -1).astype(jnp.float32)
    key_grad = k0 + one[:, :HD] + two[:, :HD]
    value_grad = v0 + one[:, HD:] + two[:, HD:]
    return layer_out, query_grad, key_grad.astype(jnp.bfloat16), value_grad.astype(jnp.bfloat16)


def solution(mesh):
    finer = Mesh(mesh.devices.reshape(16, 4, 4, 2), ("z", "x", "y", "core"))
    token = P(DP, HEAD)
    return jax.shard_map(
        on_device,
        mesh=finer,
        in_specs=(token, token, token, token, P(("y", "core", "z", "x"), None), P()),
        out_specs=(token,) * 4,
        check_vma=False,
    )
```

```python
import functools
import math

import jax
import jax.numpy as jnp
from jax import lax
from jax.experimental import pallas as pl
from jax.experimental.pallas import tpu as pltpu
from jax.sharding import Mesh
from jax.sharding import PartitionSpec as P

HD = 128
LOG2E = 1.4426950408889634
NT = (((1,), (1,)), ((), ()))
HEAD = ("y", "core")
DP = ("z", "x")
BF = jnp.bfloat16
F32 = jnp.float32
HEADS = 8


def dot_nt(a, b):
    return lax.dot_general(a, b, NT, preferred_element_type=F32)


def dot_nn(a, b):
    return jnp.dot(a, b, preferred_element_type=F32)


def call(body, name, flops, **spec):
    return pl.pallas_call(
        body,
        compiler_params=pltpu.CompilerParams(dimension_semantics=("arbitrary",) * len(spec["grid"])),
        cost_estimate=pl.CostEstimate(flops=flops, transcendentals=0, bytes_accessed=8 << 20),
        name=name,
        **spec,
    )


def forward_body(scaling, group, lengths, place, q, k2, k1, k0, v2, v1, v0, att, att_t, shares, bias, vt):
    rows = q.shape[0]
    blocks = 3

    @pl.when(pl.program_id(0) == 0)
    def _():
        first = place[0] * rows
        at = first + lax.broadcasted_iota(jnp.int32, (1, rows), 1)

        def doc(d, carry):
            end, start = carry
            end = end + lengths[d]
            return end, jnp.where(end <= at, end, start)

        _, start = lax.fori_loop(0, lengths.shape[0], doc, (jnp.int32(0), jnp.zeros((1, rows), jnp.int32)))
        keyed = first - (blocks - 1) * rows + lax.broadcasted_iota(jnp.int32, (blocks * rows, rows), 0)
        bias[...] = jnp.where((keyed >= start) & (keyed <= at), 0.0, -1e30)
        for j, v in enumerate((v2, v1, v0)):
            vt[:, j * rows : (j + 1) * rows] = v[...].T

    for h in range(group):
        cols = slice(h * HD, (h + 1) * HD)
        qh = q[:, cols]
        s = [
            dot_nt(k[...], qh) * (scaling * LOG2E) + bias[j * rows : (j + 1) * rows, :]
            for j, k in enumerate((k2, k1, k0))
        ]
        top = functools.reduce(jnp.maximum, [jnp.max(x, axis=0, keepdims=True) for x in s])
        e = [jnp.exp2(x - top) for x in s]
        inv = 1.0 / sum(jnp.sum(x, axis=0, keepdims=True) for x in e)
        out = jnp.zeros((HD, rows), F32)
        for j, x in enumerate(e):
            p = (x * inv).astype(BF)
            shares[h, j * rows : (j + 1) * rows, :] = p
            out = out + dot_nn(vt[:, j * rows : (j + 1) * rows], p)
        att_t[cols, :] = out.astype(BF)
        att[:, cols] = out.T.astype(BF)


def forward(lengths, place, q, ks, vs, group=2):
    rows, width = q.shape
    heads = width // HD
    whole = pl.BlockSpec((rows, HD), lambda i: (0, 0))
    smem = pl.BlockSpec(memory_space=pltpu.SMEM)
    return call(
        functools.partial(forward_body, 1.0 / math.sqrt(HD), group),
        "attend_forward",
        8 << 30,
        grid=(heads // group,),
        in_specs=[smem, smem, pl.BlockSpec((rows, group * HD), lambda i: (0, i))] + [whole] * 6,
        out_specs=[
            pl.BlockSpec((rows, group * HD), lambda i: (0, i)),
            pl.BlockSpec((group * HD, rows), lambda i: (i, 0)),
            pl.BlockSpec((group, 3 * rows, rows), lambda i: (i, 0, 0)),
        ],
        out_shape=[
            jax.ShapeDtypeStruct((rows, width), BF),
            jax.ShapeDtypeStruct((width, rows), BF),
            jax.ShapeDtypeStruct((heads, 3 * rows, rows), BF),
        ],
        scratch_shapes=[pltpu.VMEM((3 * rows, rows), F32), pltpu.VMEM((HD, 3 * rows), BF)],
    )(lengths, place, q, *ks, *vs)


def backward_body(scaling, group, q, k2, k1, k0, v2, v1, v0, da_own, da_far, att_t, shares, dq, far2, far1, home, kt, dka, dva):
    rows = q.shape[0]
    step = pl.program_id(0)

    @pl.when(step == 0)
    def _():
        for j, k in enumerate((k2, k1, k0)):
            kt[:, j * rows : (j + 1) * rows] = k[...].T
        dka[...] = jnp.zeros_like(dka)
        dva[...] = jnp.zeros_like(dva)

    for h in range(group):
        cols = slice(h * HD, (h + 1) * HD)
        qh = q[:, cols]
        da = (da_own[cols, :].astype(F32) + da_far[cols, :].astype(F32)).astype(BF)
        dots = jnp.sum(da.astype(F32) * att_t[cols, :].astype(F32), axis=0, keepdims=True)
        out = jnp.zeros((HD, rows), F32)
        for j, v in enumerate((v2, v1, v0)):
            own = slice(j * rows, (j + 1) * rows)
            p = shares[h, own, :]
            ds = (p.astype(F32) * (dot_nn(v[...], da) - dots)).astype(BF)
            out = out + dot_nn(kt[:, own], ds)
            dka[own, :] += dot_nn(ds, qh)
            dva[own, :] += dot_nt(p, da)
        dq[:, cols] = (out.T * scaling).astype(BF)

    @pl.when(step == pl.num_programs(0) - 1)
    def _():
        for j, to in enumerate((far2, far1, home)):
            own = slice(j * rows, (j + 1) * rows)
            to[:, :HD] = (dka[own, :] * scaling).astype(to.dtype)
            to[:, HD:] = dva[own, :].astype(to.dtype)


def backward(q, ks, vs, da_own, da_far, att_t, shares, group=2):
    rows, width = q.shape
    heads = width // HD
    whole = pl.BlockSpec((rows, HD), lambda i: (0, 0))
    head = pl.BlockSpec((rows, group * HD), lambda i: (0, i))
    head_t = pl.BlockSpec((group * HD, rows), lambda i: (i, 0))
    pair = pl.BlockSpec((rows, 2 * HD), lambda i: (0, 0))
    return call(
        functools.partial(backward_body, 1.0 / math.sqrt(HD), group),
        "attend_backward",
        8 << 30,
        grid=(heads // group,),
        in_specs=[head] + [whole] * 6 + [head_t] * 3 + [pl.BlockSpec((group, 3 * rows, rows), lambda i: (i, 0, 0))],
        out_specs=[head] + [pair] * 3,
        out_shape=[jax.ShapeDtypeStruct((rows, width), BF)]
        + [jax.ShapeDtypeStruct((rows, 2 * HD), t) for t in (BF, BF, F32)],
        scratch_shapes=[
            pltpu.VMEM((HD, 3 * rows), BF),
            pltpu.VMEM((3 * rows, HD), F32),
            pltpu.VMEM((3 * rows, HD), F32),
        ],
    )(q, *ks, *vs, da_own, da_far, att_t, shares)


def back_body(og, w, out, rhs):
    @pl.when(pl.program_id(0) == 0)
    def _():
        width = og.shape[2]
        for h in range(og.shape[0]):
            rhs[:, h * width : (h + 1) * width] = og[h]

    out[...] = dot_nt(w[...], rhs[...]).astype(out.dtype)


def project_back(og, w, which, block=256):
    heads, tokens, width = og.shape
    tokens //= 2
    rows, columns = w.shape
    return call(
        back_body,
        "project_back",
        2 << 30,
        grid=(rows // block,),
        in_specs=[
            pl.BlockSpec((heads, tokens, width), lambda i: (0, which, 0)),
            pl.BlockSpec((block, columns), lambda i: (i, 0)),
        ],
        out_specs=pl.BlockSpec((block, tokens), lambda i: (i, 0)),
        out_shape=jax.ShapeDtypeStruct((rows, tokens), BF),
        scratch_shapes=[pltpu.VMEM((tokens, columns), BF)],
    )(og, w)


def out_body(side, own, far, w, *refs):
    out, lhs = refs[-2:]

    @pl.when(pl.program_id(0) == 0)
    def _():
        rows = own.shape[0]
        lhs[:rows, :] = own[...]
        lhs[rows:, :] = far[...]

    done = dot_nn(lhs[...], w[...])
    if len(refs) == 3:
        done = done + refs[0][0].astype(F32)
    out[0] = done.astype(out.dtype)


def project_out(side, own, far, w, *add):
    rows, inner = own.shape
    width = w.shape[1] // HEADS
    whole = pl.BlockSpec((rows, inner), lambda i, s: (0, 0))
    part = pl.BlockSpec((1, 2 * rows, width), lambda i, s: (i, 0, 0))
    return pl.pallas_call(
        out_body,
        grid_spec=pltpu.PrefetchScalarGridSpec(
            num_scalar_prefetch=1,
            grid=(HEADS // 2,),
            in_specs=[whole, whole, pl.BlockSpec((inner, width), lambda i, s: (0, 2 * i + s[0]))] + [part] * len(add),
            out_specs=part,
            scratch_shapes=[pltpu.VMEM((2 * rows, inner), BF)],
        ),
        out_shape=jax.ShapeDtypeStruct((HEADS // 2, 2 * rows, width), BF),
        compiler_params=pltpu.CompilerParams(dimension_semantics=("arbitrary",)),
        cost_estimate=pl.CostEstimate(flops=2 << 30, transcendentals=0, bytes_accessed=8 << 20),
        name="project_out",
    )(side, own, far, w, *add)


def swap(pieces, axis):
    return lax.all_to_all(pieces, axis, 0, 0, tiled=True)


def everywhere(x, axis):
    return swap(jnp.broadcast_to(x[None], (lax.axis_size(axis), *x.shape)), axis)


def shifted(block, distance):
    size = lax.axis_size(DP)
    return lax.ppermute(block, DP, [(i, i + distance) for i in range(size) if 0 <= i + distance < size])


def partner(block, axis):
    return lax.ppermute(block, axis, [(i, i ^ 1) for i in range(lax.axis_size(axis))])


def on_device(queries, keys, values, output_grad, out_weight, lengths):
    rows = queries.shape[0]
    half = output_grad.shape[1] // 2
    place = lax.axis_index(DP).astype(jnp.int32).reshape(1)
    parity = lax.axis_index("x") % 2
    core = lax.axis_index("core").astype(jnp.int32).reshape(1)
    own_w = out_weight.reshape(out_weight.shape[0], HEADS, 2, half).transpose(2, 0, 1, 3)
    own_w = own_w.reshape(2, out_weight.shape[0], HEADS * half)
    own_w = swap(jnp.concatenate([own_w, own_w], axis=0), "x").reshape(-1, HEADS * half)
    weight = lax.all_gather(own_w, "z", axis=0, tiled=True)
    pair = jnp.concatenate([keys, values], axis=1)
    earlier = [shifted(pair, offset) for offset in (2, 1)]
    low, high = output_grad[:, :half], output_grad[:, half:]
    even = parity == 0
    grads = jnp.concatenate([jnp.where(even, low, high), partner(jnp.where(even, high, low), "x")], axis=0)
    grads = everywhere(grads, HEAD)
    ks = [e[:, :HD] for e in earlier] + [keys]
    vs = [e[:, HD:] for e in earlier] + [values]
    attended, attended_t, shares = forward(lengths, place, queries, ks, vs)
    attended_far = partner(attended, "x")

    d_far = partner(project_back(grads, weight, 1), "x")
    outward = partner(project_out(1 - core, attended, attended_far, weight), "core")
    d_own = project_back(grads, weight, 0)
    projected = swap(project_out(core, attended, attended_far, weight, outward), "y")
    projected = projected.astype(F32).sum(axis=0).astype(BF)
    mine = projected[:rows]
    theirs = partner(projected[rows:], "x")
    layer_out = jnp.concatenate([jnp.where(even, mine, theirs), jnp.where(even, theirs, mine)], axis=1)
    query_grad, far2, far1, home = backward(queries, ks, vs, d_own, d_far, attended_t, shares)
    total = home + shifted(far2, -2).astype(F32) + shifted(far1, -1).astype(F32)
    total = total.astype(BF)
    return layer_out, query_grad, total[:, :HD], total[:, HD:]


def solution(mesh):
    finer = Mesh(mesh.devices.reshape(16, 4, 4, 2), ("z", "x", "y", "core"))
    token = P(DP, HEAD)
    return jax.shard_map(
        on_device,
        mesh=finer,
        in_specs=(token, token, token, token, P(("y", "core", "z", "x"), None), P()),
        out_specs=(token,) * 4,
        check_vma=False,
    )
```

```python
import functools
import math

import jax
import jax.numpy as jnp
from jax import lax
from jax.experimental import pallas as pl
from jax.experimental.pallas import tpu as pltpu
from jax.sharding import Mesh
from jax.sharding import PartitionSpec as P

HD = 128
LOG2E = 1.4426950408889634
NT = (((1,), (1,)), ((), ()))
HEAD = ("y", "core")
DP = ("z_far", "z_pair", "x")
BF = jnp.bfloat16
F32 = jnp.float32
HEADS = 8


def dot_nt(a, b):
    return lax.dot_general(a, b, NT, preferred_element_type=F32)


def dot_nn(a, b):
    return jnp.dot(a, b, preferred_element_type=F32)


def call(body, name, flops, **spec):
    return pl.pallas_call(
        body,
        compiler_params=pltpu.CompilerParams(dimension_semantics=("arbitrary",) * len(spec["grid"])),
        cost_estimate=pl.CostEstimate(flops=flops, transcendentals=0, bytes_accessed=8 << 20),
        name=name,
        **spec,
    )


def forward_body(scaling, group, lengths, place, q, k2, k1, k0, v2, v1, v0, att, shares, bias, vt):
    rows = q.shape[0]
    blocks = 3

    @pl.when(pl.program_id(0) == 0)
    def _():
        first = place[0] * rows
        at = first + lax.broadcasted_iota(jnp.int32, (1, rows), 1)

        def doc(d, carry):
            end, start = carry
            end = end + lengths[d]
            return end, jnp.where(end <= at, end, start)

        _, start = lax.fori_loop(0, lengths.shape[0], doc, (jnp.int32(0), jnp.zeros((1, rows), jnp.int32)))
        keyed = first - (blocks - 1) * rows + lax.broadcasted_iota(jnp.int32, (blocks * rows, rows), 0)
        bias[...] = jnp.where((keyed >= start) & (keyed <= at), 0.0, -1e30)
        for j, v in enumerate((v2, v1, v0)):
            vt[:, j * rows : (j + 1) * rows] = v[...].T

    for h in range(group):
        cols = slice(h * HD, (h + 1) * HD)
        qh = q[:, cols]
        s = [
            dot_nt(k[...], qh) * (scaling * LOG2E) + bias[j * rows : (j + 1) * rows, :]
            for j, k in enumerate((k2, k1, k0))
        ]
        top = functools.reduce(jnp.maximum, [jnp.max(x, axis=0, keepdims=True) for x in s])
        e = [jnp.exp2(x - top) for x in s]
        inv = 1.0 / sum(jnp.sum(x, axis=0, keepdims=True) for x in e)
        out = jnp.zeros((HD, rows), F32)
        for j, x in enumerate(e):
            p = (x * inv).astype(BF)
            shares[h, j * rows : (j + 1) * rows, :] = p
            out = out + dot_nn(vt[:, j * rows : (j + 1) * rows], p)
        att[:, cols] = out.T.astype(BF)


def pair_specs(rows):
    key, value = pl.BlockSpec((rows, HD), lambda i: (0, 0)), pl.BlockSpec((rows, HD), lambda i: (1, 0))
    return [key] * 3 + [value] * 3


def forward(lengths, place, q, pairs, group=2):
    rows, width = q.shape
    heads = width // HD
    smem = pl.BlockSpec(memory_space=pltpu.SMEM)
    return call(
        functools.partial(forward_body, 1.0 / math.sqrt(HD), group),
        "attend_forward",
        8 << 30,
        grid=(heads // group,),
        in_specs=[smem, smem, pl.BlockSpec((rows, group * HD), lambda i: (0, i))] + pair_specs(rows),
        out_specs=[
            pl.BlockSpec((rows, group * HD), lambda i: (0, i)),
            pl.BlockSpec((group, 3 * rows, rows), lambda i: (i, 0, 0)),
        ],
        out_shape=[
            jax.ShapeDtypeStruct((rows, width), BF),
            jax.ShapeDtypeStruct((heads, 3 * rows, rows), BF),
        ],
        scratch_shapes=[pltpu.VMEM((3 * rows, rows), F32), pltpu.VMEM((HD, 3 * rows), BF)],
    )(lengths, place, q, *pairs, *pairs)


def backward_body(scaling, group, q, k2, k1, k0, v2, v1, v0, d0, d1, d2, d3, att, shares, dq, far2, far1, home, kt, dka, dva):
    rows = q.shape[0]
    step = pl.program_id(0)

    @pl.when(step == 0)
    def _():
        for j, k in enumerate((k2, k1, k0)):
            kt[:, j * rows : (j + 1) * rows] = k[...].T
        dka[...] = jnp.zeros_like(dka)
        dva[...] = jnp.zeros_like(dva)

    for h in range(group):
        cols = slice(h * HD, (h + 1) * HD)
        qh = q[:, cols]
        da = sum(d[:, cols].astype(F32) for d in (d0, d1, d2, d3)).astype(BF)
        prod = da.astype(F32) * att[:, cols].astype(F32)
        dots = jnp.sum(prod.T, axis=0, keepdims=True)
        out = jnp.zeros((HD, rows), F32)
        for j, v in enumerate((v2, v1, v0)):
            own = slice(j * rows, (j + 1) * rows)
            p = shares[h, own, :]
            ds = (p.astype(F32) * (dot_nt(v[...], da) - dots)).astype(BF)
            out = out + dot_nn(kt[:, own], ds)
            dka[own, :] += dot_nn(ds, qh)
            dva[own, :] += dot_nn(p, da)
        dq[:, cols] = (out.T * scaling).astype(BF)

    @pl.when(step == pl.num_programs(0) - 1)
    def _():
        for j, to in enumerate((far2, far1, home)):
            own = slice(j * rows, (j + 1) * rows)
            to[:rows, :] = (dka[own, :] * scaling).astype(to.dtype)
            to[rows:, :] = dva[own, :].astype(to.dtype)


def backward(q, pairs, d_parts, att, shares, group=2):
    rows, width = q.shape
    heads = width // HD
    head = pl.BlockSpec((rows, group * HD), lambda i: (0, i))
    pair = pl.BlockSpec((2 * rows, HD), lambda i: (0, 0))
    return call(
        functools.partial(backward_body, 1.0 / math.sqrt(HD), group),
        "attend_backward",
        8 << 30,
        grid=(heads // group,),
        in_specs=[head]
        + pair_specs(rows)
        + [head] * (len(d_parts) + 1)
        + [pl.BlockSpec((group, 3 * rows, rows), lambda i: (i, 0, 0))],
        out_specs=[head] + [pair] * 3,
        out_shape=[jax.ShapeDtypeStruct((rows, width), BF)]
        + [jax.ShapeDtypeStruct((2 * rows, HD), t) for t in (BF, BF, F32)],
        scratch_shapes=[
            pltpu.VMEM((HD, 3 * rows), BF),
            pltpu.VMEM((3 * rows, HD), F32),
            pltpu.VMEM((3 * rows, HD), F32),
        ],
    )(q, *pairs, *pairs, *d_parts, att, shares)


def back_body(index, og, w, *refs):
    *outs, lhs = refs
    rows = outs[0].shape[0]

    @pl.when(pl.program_id(0) == 0)
    def _():
        for k in range(len(outs)):
            block = lax.rem(index[0] + k, len(outs))
            at = pl.ds(pl.multiple_of(block * rows, rows), rows)
            for h in range(og.shape[0]):
                lhs[k * rows : (k + 1) * rows, h * HD : (h + 1) * HD] = og[h, at, :]

    done = dot_nt(lhs[...], w[...]).astype(BF)
    for k, out in enumerate(outs):
        out[...] = done[k * rows : (k + 1) * rows]


def project_back(index, og, w, parts, block=256):
    heads, tokens, width = og.shape
    inner, columns = w.shape
    rows = tokens // parts
    return pl.pallas_call(
        back_body,
        grid_spec=pltpu.PrefetchScalarGridSpec(
            num_scalar_prefetch=1,
            grid=(inner // block,),
            in_specs=[
                pl.BlockSpec((heads, tokens, width), lambda i, s: (0, 0, 0)),
                pl.BlockSpec((block, columns), lambda i, s: (i, 0)),
            ],
            out_specs=[pl.BlockSpec((rows, block), lambda i, s: (0, i))] * parts,
            scratch_shapes=[pltpu.VMEM((tokens, columns), BF)],
        ),
        out_shape=[jax.ShapeDtypeStruct((rows, inner), BF)] * parts,
        compiler_params=pltpu.CompilerParams(dimension_semantics=("arbitrary",)),
        cost_estimate=pl.CostEstimate(flops=2 << 30, transcendentals=0, bytes_accessed=8 << 20),
        name="project_back",
    )(index, og, w)


def out_body(parts, index, *refs):
    blocks, w0, w1, add = refs[:parts], refs[parts], refs[parts + 1], refs[parts + 3 : -2]
    out, lhs = refs[-2:]
    rows = blocks[0].shape[0]

    @pl.when(pl.program_id(0) == 0)
    def _():
        for k, block in enumerate(blocks):
            owner = lax.rem(index[0] + parts - k, parts)
            lhs[pl.ds(pl.multiple_of(owner * rows, rows), rows), :] = block[...]

    done = dot_nn(lhs[...], jnp.concatenate([w0[...], w1[...]], axis=1))
    for n in range(2):
        value = done[:, n * HD : (n + 1) * HD]
        for more in add:
            value = value + more[n].astype(F32)
        out[n] = value.astype(BF)


def project_out(index, blocks, w, after, *add):
    rows, inner = blocks[0].shape
    parts = len(blocks)
    whole = pl.BlockSpec((rows, inner), lambda i, s: (0, 0))
    part = pl.BlockSpec((2, parts * rows, HD), lambda i, s: (i, 0, 0))
    columns = [pl.BlockSpec((inner, HD), lambda i, s, n=n: (0, 4 * i + 2 * n + s[1])) for n in range(2)]
    return pl.pallas_call(
        functools.partial(out_body, parts),
        grid_spec=pltpu.PrefetchScalarGridSpec(
            num_scalar_prefetch=1,
            grid=(HEADS // 4,),
            in_specs=[whole] * parts + columns + [pl.BlockSpec(memory_space=pl.ANY)] + [part] * len(add),
            out_specs=part,
            scratch_shapes=[pltpu.VMEM((parts * rows, inner), BF)],
        ),
        out_shape=jax.ShapeDtypeStruct((HEADS // 2, parts * rows, HD), BF),
        compiler_params=pltpu.CompilerParams(dimension_semantics=("arbitrary",)),
        cost_estimate=pl.CostEstimate(flops=1 << 30, transcendentals=0, bytes_accessed=4 << 20),
        name="project_out",
    )(index, *blocks, w, w, after, *add)


def swap(pieces, axis):
    return lax.all_to_all(pieces, axis, 0, 0, tiled=True)


def everywhere(x, axis):
    return swap(jnp.broadcast_to(x[None], (lax.axis_size(axis), *x.shape)), axis)


def shifted(block, distance):
    size = lax.axis_size(DP)
    return lax.ppermute(block, DP, [(i, i + distance) for i in range(size) if 0 <= i + distance < size])


def partner(block, axis):
    return lax.ppermute(block, axis, [(i, i ^ 1) for i in range(lax.axis_size(axis))])


def around(blocks, axis, step):
    size = lax.axis_size(axis)
    return [blocks[0]] + [
        lax.ppermute(blocks[k], axis, [(i, (i + k * step) % size) for i in range(size)]) for k in range(1, size)
    ]


def on_device(queries, keys, values, output_grad, out_weight, lengths):
    rows = queries.shape[0]
    few = out_weight.shape[0]
    parts = lax.axis_size("x")
    place = lax.axis_index(DP).astype(jnp.int32).reshape(1)
    index = lax.axis_index("x").astype(jnp.int32)
    core = lax.axis_index("core").astype(jnp.int32)
    own_w = out_weight.reshape(few, HEADS, parts, HD).transpose(2, 0, 1, 3).reshape(parts, few, HEADS * HD)
    own_w = jnp.concatenate([own_w] * 2, axis=0)
    own_w = swap(own_w, ("z_pair", "x")).reshape(-1, HEADS * HD)
    weight = lax.all_gather(own_w, "z_far", axis=0, tiled=True)
    pair = jnp.concatenate([keys, values], axis=0)
    pairs = [shifted(pair, 2), shifted(pair, 1), pair]
    own_g = output_grad.reshape(rows, parts, HD).transpose(1, 0, 2)
    grads = everywhere(swap(own_g, "x").reshape(parts * rows, HD), HEAD)
    attended, shares = forward(lengths, place, queries, pairs)
    attended_all = around([attended] * parts, "x", 1)

    d_here = project_back(index.reshape(1), grads, weight, parts)
    d_parts = around(d_here, "x", 1)
    outward = partner(project_out(jnp.stack([index, 1 - core]), attended_all, weight, d_here[0]), "core")
    projected = swap(project_out(jnp.stack([index, core]), attended_all, weight, d_here[0], outward), "y")
    projected = projected.astype(F32).sum(axis=0).astype(BF)
    feature_parts = swap(projected.reshape(parts, rows, HD), "x")
    query_grad, far2, far1, home = backward(queries, pairs, d_parts, attended, shares)
    two, one = shifted(far2, -2), shifted(far1, -1)
    home, feature_parts = lax.optimization_barrier((home, feature_parts))
    layer_out = jnp.concatenate([feature_parts[j] for j in range(parts)], axis=1)
    total = (home + two.astype(F32) + one.astype(F32)).astype(BF)
    return layer_out, query_grad, total[:rows], total[rows:]


def solution(mesh):
    finer = Mesh(mesh.devices.reshape(8, 2, 4, 4, 2), ("z_far", "z_pair", "x", "y", "core"))
    token = P(DP, HEAD)
    return jax.shard_map(
        on_device,
        mesh=finer,
        in_specs=(token, token, token, token, P((*HEAD, *DP), None), P()),
        out_specs=(token,) * 4,
        check_vma=False,
    )
```

```python
import functools
import math

import jax
import jax.numpy as jnp
from jax import lax
from jax.experimental import pallas as pl
from jax.experimental.pallas import tpu as pltpu
from jax.sharding import Mesh
from jax.sharding import PartitionSpec as P

HD = 128
LOG2E = 1.4426950408889634
NT = (((1,), (1,)), ((), ()))
HEAD = ("y", "core")
DP = ("z_far", "z_pair", "x")
BF = jnp.bfloat16
F32 = jnp.float32
HEADS = 8


def dot_nt(a, b):
    return lax.dot_general(a, b, NT, preferred_element_type=F32)


def dot_nn(a, b):
    return jnp.dot(a, b, preferred_element_type=F32)


def call(body, flops, **spec):
    return pl.pallas_call(
        body,
        compiler_params=pltpu.CompilerParams(dimension_semantics=("arbitrary",) * len(spec["grid"])),
        cost_estimate=pl.CostEstimate(flops=flops, transcendentals=0, bytes_accessed=8 << 20),
        **spec,
    )


def forward_body(scaling, group, lengths, place, q, k2, k1, k0, v2, v1, v0, att, shares, bias, vt):
    rows = q.shape[0]
    blocks = 3

    @pl.when(pl.program_id(0) == 0)
    def _():
        first = place[0] * rows
        at = first + lax.broadcasted_iota(jnp.int32, (1, rows), 1)

        def doc(d, carry):
            end, start = carry
            end = end + lengths[d]
            return end, jnp.where(end <= at, end, start)

        _, start = lax.fori_loop(0, lengths.shape[0], doc, (jnp.int32(0), jnp.zeros((1, rows), jnp.int32)))
        keyed = first - (blocks - 1) * rows + lax.broadcasted_iota(jnp.int32, (blocks * rows, rows), 0)
        bias[...] = jnp.where((keyed >= start) & (keyed <= at), 0.0, -1e30)
        for j, v in enumerate((v2, v1, v0)):
            vt[:, j * rows : (j + 1) * rows] = v[...].T

    for h in range(group):
        cols = slice(h * HD, (h + 1) * HD)
        qh = q[:, cols]
        s = [
            dot_nt(k[...], qh) * (scaling * LOG2E) + bias[j * rows : (j + 1) * rows, :]
            for j, k in enumerate((k2, k1, k0))
        ]
        top = functools.reduce(jnp.maximum, [jnp.max(x, axis=0, keepdims=True) for x in s])
        e = [jnp.exp2(x - top) for x in s]
        inv = 1.0 / sum(jnp.sum(x, axis=0, keepdims=True) for x in e)
        out = jnp.zeros((HD, rows), F32)
        for j, x in enumerate(e):
            p = (x * inv).astype(BF)
            shares[h, j * rows : (j + 1) * rows, :] = p
            out = out + dot_nn(vt[:, j * rows : (j + 1) * rows], p)
        att[:, cols] = out.T.astype(BF)


def pair_specs(rows):
    key, value = pl.BlockSpec((rows, HD), lambda i: (0, 0)), pl.BlockSpec((rows, HD), lambda i: (1, 0))
    return [key] * 3 + [value] * 3


def forward(lengths, place, q, pairs, group=2):
    rows, width = q.shape
    heads = width // HD
    smem = pl.BlockSpec(memory_space=pltpu.SMEM)
    return call(
        functools.partial(forward_body, 1.0 / math.sqrt(HD), group),
        8 << 30,
        grid=(heads // group,),
        in_specs=[smem, smem, pl.BlockSpec((rows, group * HD), lambda i: (0, i))] + pair_specs(rows),
        out_specs=[
            pl.BlockSpec((rows, group * HD), lambda i: (0, i)),
            pl.BlockSpec((group, 3 * rows, rows), lambda i: (i, 0, 0)),
        ],
        out_shape=[
            jax.ShapeDtypeStruct((rows, width), BF),
            jax.ShapeDtypeStruct((heads, 3 * rows, rows), BF),
        ],
        scratch_shapes=[pltpu.VMEM((3 * rows, rows), F32), pltpu.VMEM((HD, 3 * rows), BF)],
    )(lengths, place, q, *pairs, *pairs)


def backward_body(scaling, group, q, k2, k1, k0, v2, v1, v0, d0, d1, d2, d3, att, shares, dq, far2, far1, home, kt, dka, dva):
    rows = q.shape[0]
    step = pl.program_id(0)

    @pl.when(step == 0)
    def _():
        for j, k in enumerate((k2, k1, k0)):
            kt[:, j * rows : (j + 1) * rows] = k[...].T
        dka[...] = jnp.zeros_like(dka)
        dva[...] = jnp.zeros_like(dva)

    spans = [slice(h * HD, (h + 1) * HD) for h in range(group)]
    das = [sum(d[:, cols].astype(F32) for d in (d0, d1, d2, d3)).astype(BF) for cols in spans]
    prods = [da.astype(F32) * att[:, cols].astype(F32) for da, cols in zip(das, spans)]
    dots = [jnp.sum(prod.T, axis=0, keepdims=True) for prod in prods]
    stacked_q = jnp.concatenate([q[:, cols] for cols in spans], axis=0)
    stacked_da = jnp.concatenate(das, axis=0)
    outs = [jnp.zeros((HD, rows), F32)] * group
    for j, v in enumerate((v2, v1, v0)):
        own = slice(j * rows, (j + 1) * rows)
        low = [shares[h, own, :] for h in range(group)]
        ds = [(p.astype(F32) * (dot_nt(v[...], da) - dot)).astype(BF) for p, da, dot in zip(low, das, dots)]
        outs = [out + dot_nn(kt[:, own], d) for out, d in zip(outs, ds)]
        dka[own, :] += dot_nn(jnp.concatenate(ds, axis=1), stacked_q)
        dva[own, :] += dot_nn(jnp.concatenate(low, axis=1), stacked_da)
    for cols, out in zip(spans, outs):
        dq[:, cols] = (out.T * scaling).astype(BF)

    @pl.when(step == pl.num_programs(0) - 1)
    def _():
        for j, to in enumerate((far2, far1, home)):
            own = slice(j * rows, (j + 1) * rows)
            to[:rows, :] = (dka[own, :] * scaling).astype(to.dtype)
            to[rows:, :] = dva[own, :].astype(to.dtype)


def backward(q, pairs, d_parts, att, shares, group=2):
    rows, width = q.shape
    heads = width // HD
    head = pl.BlockSpec((rows, group * HD), lambda i: (0, i))
    pair = pl.BlockSpec((2 * rows, HD), lambda i: (0, 0))
    return call(
        functools.partial(backward_body, 1.0 / math.sqrt(HD), group),
        8 << 30,
        grid=(heads // group,),
        in_specs=[head]
        + pair_specs(rows)
        + [head] * (len(d_parts) + 1)
        + [pl.BlockSpec((group, 3 * rows, rows), lambda i: (i, 0, 0))],
        out_specs=[head] + [pair] * 3,
        out_shape=[jax.ShapeDtypeStruct((rows, width), BF)]
        + [jax.ShapeDtypeStruct((2 * rows, HD), t) for t in (BF, BF, F32)],
        scratch_shapes=[
            pltpu.VMEM((HD, 3 * rows), BF),
            pltpu.VMEM((3 * rows, HD), F32),
            pltpu.VMEM((3 * rows, HD), F32),
        ],
    )(q, *pairs, *pairs, *d_parts, att, shares)


def back_body(index, og, w, *refs):
    *outs, lhs = refs
    rows = outs[0].shape[0]

    @pl.when(pl.program_id(0) == 0)
    def _():
        for k in range(len(outs)):
            block = lax.rem(index[0] + k, len(outs))
            at = pl.ds(pl.multiple_of(block * rows, rows), rows)
            for h in range(og.shape[0]):
                lhs[k * rows : (k + 1) * rows, h * HD : (h + 1) * HD] = og[h, at, :]

    done = dot_nt(lhs[...], w[...]).astype(BF)
    for k, out in enumerate(outs):
        out[...] = done[k * rows : (k + 1) * rows]


def project_back(index, og, w, parts, block=256):
    _, tokens, _ = og.shape
    inner, columns = w.shape
    rows = tokens // parts
    return pl.pallas_call(
        back_body,
        grid_spec=pltpu.PrefetchScalarGridSpec(
            num_scalar_prefetch=1,
            grid=(inner // block,),
            in_specs=[
                pl.BlockSpec(memory_space=pltpu.VMEM),
                pl.BlockSpec((block, columns), lambda i, s: (i, 0)),
            ],
            out_specs=[pl.BlockSpec((rows, block), lambda i, s: (0, i))] * parts,
            scratch_shapes=[pltpu.VMEM((tokens, columns), BF)],
        ),
        out_shape=[jax.ShapeDtypeStruct((rows, inner), BF)] * parts,
        compiler_params=pltpu.CompilerParams(dimension_semantics=("arbitrary",)),
        cost_estimate=pl.CostEstimate(flops=2 << 30, transcendentals=0, bytes_accessed=8 << 20),
        name="project_back",
    )(index, og, w)


def out_body(parts, index, side, *refs):
    blocks, w0, w1, add = refs[:parts], refs[parts], refs[parts + 1], refs[parts + 3 : -2]
    out, lhs = refs[-2:]
    rows = blocks[0].shape[0]

    @pl.when(pl.program_id(0) == 0)
    def _():
        for k, block in enumerate(blocks):
            owner = lax.rem(index[0] + parts - k, parts)
            lhs[pl.ds(pl.multiple_of(owner * rows, rows), rows), :] = block[...]

    done = dot_nn(lhs[...], jnp.concatenate([w0[...], w1[...]], axis=1))
    for n in range(2):
        value = done[:, n * HD : (n + 1) * HD]
        for more in add:
            value = value + more[2 * pl.program_id(0) + n].astype(F32)
        out[n] = value.astype(BF)


def project_out(index, side, blocks, w, after, *add):
    rows, inner = blocks[0].shape
    parts = len(blocks)
    whole = pl.BlockSpec(memory_space=pltpu.VMEM)
    part = pl.BlockSpec((2, parts * rows, HD), lambda i, x, s: (i, 0, 0))
    columns = [pl.BlockSpec((inner, HD), lambda i, x, s, n=n: (0, 4 * i + 2 * n + s[0])) for n in range(2)]
    return pl.pallas_call(
        functools.partial(out_body, parts),
        grid_spec=pltpu.PrefetchScalarGridSpec(
            num_scalar_prefetch=2,
            grid=(HEADS // 4,),
            in_specs=[whole] * parts + columns + [pl.BlockSpec(memory_space=pl.ANY)] + [whole] * len(add),
            out_specs=part,
            scratch_shapes=[pltpu.VMEM((parts * rows, inner), BF)],
        ),
        out_shape=jax.ShapeDtypeStruct((HEADS // 2, parts * rows, HD), BF),
        compiler_params=pltpu.CompilerParams(dimension_semantics=("arbitrary",)),
        cost_estimate=pl.CostEstimate(flops=1 << 30, transcendentals=0, bytes_accessed=4 << 20),
        name="project_out",
    )(index, side, *blocks, w, w, after, *add)


def swap(pieces, axis):
    return lax.all_to_all(pieces, axis, 0, 0, tiled=True)


def everywhere(x, axis):
    return swap(jnp.broadcast_to(x[None], (lax.axis_size(axis), *x.shape)), axis)


def shifted(block, distance):
    size = lax.axis_size(DP)
    return lax.ppermute(block, DP, [(i, i + distance) for i in range(size) if 0 <= i + distance < size])


def partner(block, axis):
    return lax.ppermute(block, axis, [(i, i ^ 1) for i in range(lax.axis_size(axis))])


def around(blocks, axis, step):
    size = lax.axis_size(axis)
    return [blocks[0]] + [
        lax.ppermute(blocks[k], axis, [(i, (i + k * step) % size) for i in range(size)]) for k in range(1, size)
    ]


def on_device(queries, keys, values, output_grad, out_weight, lengths):
    rows = queries.shape[0]
    few = out_weight.shape[0]
    parts = lax.axis_size("x")
    place = lax.axis_index(DP).astype(jnp.int32).reshape(1)
    index = lax.axis_index("x").astype(jnp.int32).reshape(1)
    core = lax.axis_index("core").astype(jnp.int32).reshape(1)
    own_w = out_weight.reshape(few, HEADS, parts, HD).transpose(2, 0, 1, 3).reshape(parts, few, HEADS * HD)
    own_w = jnp.concatenate([own_w] * 2, axis=0)
    own_w = swap(own_w, ("z_pair", "x")).reshape(-1, HEADS * HD)
    weight = lax.all_gather(own_w, "z_far", axis=0, tiled=True)
    pair = jnp.concatenate([keys, values], axis=0)
    pairs = [shifted(pair, 2), shifted(pair, 1), pair]
    own_g = output_grad.reshape(rows, parts, HD).transpose(1, 0, 2)
    grads = swap(own_g, "x").reshape(parts * rows, HD)
    grads = everywhere(grads, HEAD)
    attended, shares = forward(lengths, place, queries, pairs)
    attended_all = around([attended] * parts, "x", 1)

    d_here = project_back(index, grads, weight, parts)
    d_parts = around(d_here, "x", 1)
    outward = project_out(index, 1 - core, attended_all, weight, d_here[0])
    outward = partner(outward, "core")
    projected = project_out(index, core, attended_all, weight, d_here[0], outward)
    projected = swap(projected, "y")
    projected = projected.astype(F32).sum(axis=0).astype(BF)
    feature_parts = swap(projected.reshape(parts, rows, HD), "x")
    query_grad, far2, far1, home = backward(queries, pairs, d_parts, attended, shares)
    two, one = shifted(far2, -2), shifted(far1, -1)
    home, feature_parts = lax.optimization_barrier((home, feature_parts))
    layer_out = jnp.concatenate([feature_parts[j] for j in range(parts)], axis=1)
    total = (home + two.astype(F32) + one.astype(F32)).astype(BF)
    return layer_out, query_grad, total[:rows], total[rows:]


def solution(mesh):
    finer = Mesh(mesh.devices.reshape(8, 2, 4, 4, 2), ("z_far", "z_pair", "x", "y", "core"))
    token = P(DP, HEAD)

    return jax.shard_map(
        on_device,
        mesh=finer,
        in_specs=(token, token, token, token, P((*HEAD, *DP), None), P()),
        out_specs=(token,) * 4,
        check_vma=False,
    )
```

```python
import functools
import math

import jax
import jax.numpy as jnp
from jax import lax
from jax.experimental import pallas as pl
from jax.experimental.pallas import tpu as pltpu
from jax.sharding import Mesh
from jax.sharding import PartitionSpec as P

HD = 128
LOG2E = 1.4426950408889634
NT = (((1,), (1,)), ((), ()))
HEAD = ("y", "core")
DP = ("z_far", "z_pair", "x")
BF = jnp.bfloat16
F32 = jnp.float32
HEADS = 8


def dot_nt(a, b):
    return lax.dot_general(a, b, NT, preferred_element_type=F32)


def dot_nn(a, b):
    return jnp.dot(a, b, preferred_element_type=F32)


def call(body, flops, **spec):
    return pl.pallas_call(
        body,
        compiler_params=pltpu.CompilerParams(dimension_semantics=("arbitrary",) * len(spec["grid"])),
        cost_estimate=pl.CostEstimate(flops=flops, transcendentals=0, bytes_accessed=8 << 20),
        **spec,
    )


def forward_body(scaling, group, lengths, place, q, k2, k1, k0, v2, v1, v0, att, shares, bias, vt):
    rows = q.shape[0]
    blocks = 3

    @pl.when(pl.program_id(0) == 0)
    def _():
        first = place[0] * rows
        at = first + lax.broadcasted_iota(jnp.int32, (1, rows), 1)

        def doc(d, carry):
            end, start = carry
            end = end + lengths[d]
            return end, jnp.where(end <= at, end, start)

        _, start = lax.fori_loop(0, lengths.shape[0], doc, (jnp.int32(0), jnp.zeros((1, rows), jnp.int32)))
        keyed = first - (blocks - 1) * rows + lax.broadcasted_iota(jnp.int32, (blocks * rows, rows), 0)
        bias[...] = jnp.where((keyed >= start) & (keyed <= at), 0.0, -1e30)
        for j, v in enumerate((v2, v1, v0)):
            vt[:, j * rows : (j + 1) * rows] = v[...].T

    for h in range(group):
        cols = slice(h * HD, (h + 1) * HD)
        qh = q[:, cols]
        s = [
            dot_nt(k[...], qh) * (scaling * LOG2E) + bias[j * rows : (j + 1) * rows, :]
            for j, k in enumerate((k2, k1, k0))
        ]
        top = functools.reduce(jnp.maximum, [jnp.max(x, axis=0, keepdims=True) for x in s])
        e = [jnp.exp2(x - top) for x in s]
        inv = 1.0 / sum(jnp.sum(x, axis=0, keepdims=True) for x in e)
        out = jnp.zeros((HD, rows), F32)
        for j, x in enumerate(e):
            p = (x * inv).astype(BF)
            shares[h, j * rows : (j + 1) * rows, :] = p
            out = out + dot_nn(vt[:, j * rows : (j + 1) * rows], p)
        att[:, cols] = out.T.astype(BF)


def pair_specs(rows):
    key, value = pl.BlockSpec((rows, HD), lambda i: (0, 0)), pl.BlockSpec((rows, HD), lambda i: (1, 0))
    return [key] * 3 + [value] * 3


def forward(lengths, place, q, pairs, group=2):
    rows, width = q.shape
    heads = width // HD
    smem = pl.BlockSpec(memory_space=pltpu.SMEM)
    return call(
        functools.partial(forward_body, 1.0 / math.sqrt(HD), group),
        8 << 30,
        grid=(heads // group,),
        in_specs=[smem, smem, pl.BlockSpec((rows, group * HD), lambda i: (0, i))] + pair_specs(rows),
        out_specs=[
            pl.BlockSpec((rows, group * HD), lambda i: (0, i)),
            pl.BlockSpec((group, 3 * rows, rows), lambda i: (i, 0, 0)),
        ],
        out_shape=[
            jax.ShapeDtypeStruct((rows, width), BF),
            jax.ShapeDtypeStruct((heads, 3 * rows, rows), BF),
        ],
        scratch_shapes=[pltpu.VMEM((3 * rows, rows), F32), pltpu.VMEM((HD, 3 * rows), BF)],
    )(lengths, place, q, *pairs, *pairs)


def backward_body(scaling, group, q, k2, k1, k0, v2, v1, v0, d_parts, att, shares, dq, far2, far1, home, kt, dka, dva):
    rows = q.shape[0]
    step = pl.program_id(0)

    @pl.when(step == 0)
    def _():
        for j, k in enumerate((k2, k1, k0)):
            kt[:, j * rows : (j + 1) * rows] = k[...].T
        dka[...] = jnp.zeros_like(dka)
        dva[...] = jnp.zeros_like(dva)

    spans = [slice(h * HD, (h + 1) * HD) for h in range(group)]
    das = [sum(d_parts[i, :, cols].astype(F32) for i in range(d_parts.shape[0])).astype(BF) for cols in spans]
    prods = [da.astype(F32) * att[:, cols].astype(F32) for da, cols in zip(das, spans)]
    dots = [jnp.sum(prod.T, axis=0, keepdims=True) for prod in prods]
    stacked_q = jnp.concatenate([q[:, cols] for cols in spans], axis=0)
    stacked_da = jnp.concatenate(das, axis=0)
    outs = [jnp.zeros((HD, rows), F32)] * group
    for j, v in enumerate((v2, v1, v0)):
        own = slice(j * rows, (j + 1) * rows)
        low = [shares[h, own, :] for h in range(group)]
        ds = [(p.astype(F32) * (dot_nt(v[...], da) - dot)).astype(BF) for p, da, dot in zip(low, das, dots)]
        outs = [out + dot_nn(kt[:, own], d) for out, d in zip(outs, ds)]
        dka[own, :] += dot_nn(jnp.concatenate(ds, axis=1), stacked_q)
        dva[own, :] += dot_nn(jnp.concatenate(low, axis=1), stacked_da)
    for cols, out in zip(spans, outs):
        dq[:, cols] = (out.T * scaling).astype(BF)

    @pl.when(step == pl.num_programs(0) - 1)
    def _():
        for j, to in enumerate((far2, far1, home)):
            own = slice(j * rows, (j + 1) * rows)
            to[:rows, :] = (dka[own, :] * scaling).astype(to.dtype)
            to[rows:, :] = dva[own, :].astype(to.dtype)


def backward(q, pairs, d_parts, att, shares, group=2):
    rows, width = q.shape
    heads = width // HD
    head = pl.BlockSpec((rows, group * HD), lambda i: (0, i))
    pair = pl.BlockSpec((2 * rows, HD), lambda i: (0, 0))
    return call(
        functools.partial(backward_body, 1.0 / math.sqrt(HD), group),
        8 << 30,
        grid=(heads // group,),
        in_specs=[head]
        + pair_specs(rows)
        + [pl.BlockSpec((d_parts.shape[0], rows, group * HD), lambda i: (0, 0, i)), head]
        + [pl.BlockSpec((group, 3 * rows, rows), lambda i: (i, 0, 0))],
        out_specs=[head] + [pair] * 3,
        out_shape=[jax.ShapeDtypeStruct((rows, width), BF)]
        + [jax.ShapeDtypeStruct((2 * rows, HD), t) for t in (BF, BF, F32)],
        scratch_shapes=[
            pltpu.VMEM((HD, 3 * rows), BF),
            pltpu.VMEM((3 * rows, HD), F32),
            pltpu.VMEM((3 * rows, HD), F32),
        ],
    )(q, *pairs, *pairs, d_parts, att, shares)


def back_body(og, w, out, lhs):
    @pl.when(pl.program_id(0) == 0)
    def _():
        for h in range(og.shape[0]):
            lhs[:, h * HD : (h + 1) * HD] = og[h]

    rows = out.shape[1]
    done = dot_nt(lhs[...], w[...]).astype(BF)
    for b in range(out.shape[0]):
        out[b] = done[b * rows : (b + 1) * rows]


def project_back(og, w, parts, block=256):
    _, tokens, _ = og.shape
    inner, columns = w.shape
    rows = tokens // parts
    return call(
        back_body,
        2 << 30,
        grid=(inner // block,),
        in_specs=[pl.BlockSpec(memory_space=pltpu.VMEM), pl.BlockSpec((block, columns), lambda i: (i, 0))],
        out_specs=pl.BlockSpec((parts, rows, block), lambda i: (0, 0, i)),
        out_shape=jax.ShapeDtypeStruct((parts, rows, inner), BF),
        scratch_shapes=[pltpu.VMEM((tokens, columns), BF)],
    )(og, w)


def out_body(parts, index, side, *refs):
    blocks, w0, w1, add = refs[:parts], refs[parts], refs[parts + 1], refs[parts + 3 : -2]
    out, lhs = refs[-2:]
    rows = blocks[0].shape[0]

    @pl.when(pl.program_id(0) == 0)
    def _():
        for k, block in enumerate(blocks):
            owner = lax.rem(index[0] + parts - k, parts)
            lhs[pl.ds(pl.multiple_of(owner * rows, rows), rows), :] = block[...]

    done = dot_nn(lhs[...], jnp.concatenate([w0[...], w1[...]], axis=1))
    for n in range(2):
        value = done[:, n * HD : (n + 1) * HD]
        for more in add:
            value = value + more[2 * pl.program_id(0) + n].astype(F32)
        out[n] = value.astype(BF)


def project_out(index, side, blocks, w, after, *add):
    rows, inner = blocks[0].shape
    parts = len(blocks)
    whole = pl.BlockSpec(memory_space=pltpu.VMEM)
    part = pl.BlockSpec((2, parts * rows, HD), lambda i, x, s: (i, 0, 0))
    columns = [pl.BlockSpec((inner, HD), lambda i, x, s, n=n: (0, 4 * i + 2 * n + s[0])) for n in range(2)]
    return pl.pallas_call(
        functools.partial(out_body, parts),
        grid_spec=pltpu.PrefetchScalarGridSpec(
            num_scalar_prefetch=2,
            grid=(HEADS // 4,),
            in_specs=[whole] * parts + columns + [pl.BlockSpec(memory_space=pl.ANY)] + [whole] * len(add),
            out_specs=part,
            scratch_shapes=[pltpu.VMEM((parts * rows, inner), BF)],
        ),
        out_shape=jax.ShapeDtypeStruct((HEADS // 2, parts * rows, HD), BF),
        compiler_params=pltpu.CompilerParams(dimension_semantics=("arbitrary",)),
        cost_estimate=pl.CostEstimate(flops=1 << 30, transcendentals=0, bytes_accessed=4 << 20),
        name="project_out",
    )(index, side, *blocks, w, w, after, *add)


def swap(pieces, axis):
    return lax.all_to_all(pieces, axis, 0, 0, tiled=True)


def everywhere(x, axis):
    return swap(jnp.broadcast_to(x[None], (lax.axis_size(axis), *x.shape)), axis)


def shifted(block, distance):
    size = lax.axis_size(DP)
    return lax.ppermute(block, DP, [(i, i + distance) for i in range(size) if 0 <= i + distance < size])


def partner(block, axis):
    return lax.ppermute(block, axis, [(i, i ^ 1) for i in range(lax.axis_size(axis))])


def around(blocks, axis, step):
    size = lax.axis_size(axis)
    return [blocks[0]] + [
        lax.ppermute(blocks[k], axis, [(i, (i + k * step) % size) for i in range(size)]) for k in range(1, size)
    ]


def on_device(queries, keys, values, output_grad, out_weight, lengths):
    rows = queries.shape[0]
    few = out_weight.shape[0]
    parts = lax.axis_size("x")
    place = lax.axis_index(DP).astype(jnp.int32).reshape(1)
    index = lax.axis_index("x").astype(jnp.int32).reshape(1)
    core = lax.axis_index("core").astype(jnp.int32).reshape(1)
    own_w = out_weight.reshape(few, HEADS, parts, HD).transpose(2, 0, 1, 3).reshape(parts, few, HEADS * HD)
    own_w = jnp.concatenate([own_w] * 2, axis=0)
    own_w = swap(own_w, ("z_pair", "x")).reshape(-1, HEADS * HD)
    weight = lax.all_gather(own_w, "z_far", axis=0, tiled=True)
    pair = jnp.concatenate([keys, values], axis=0)
    pairs = [shifted(pair, 2), shifted(pair, 1), pair]
    own_g = output_grad.reshape(rows, parts, HD).transpose(1, 0, 2)
    grads = swap(own_g, "x").reshape(parts * rows, HD)
    grads = everywhere(grads, HEAD)
    attended, shares = forward(lengths, place, queries, pairs)
    attended_all = around([attended] * parts, "x", 1)

    d_here = project_back(grads, weight, parts)
    d_parts = swap(d_here, "x")
    outward = project_out(index, 1 - core, attended_all, weight, d_here)
    outward = partner(outward, "core")
    projected = project_out(index, core, attended_all, weight, d_here, outward)
    projected = swap(projected, "y")
    projected = projected.astype(F32).sum(axis=0).astype(BF)
    feature_parts = swap(projected.reshape(parts, rows, HD), "x")
    query_grad, far2, far1, home = backward(queries, pairs, d_parts, attended, shares)
    two, one = shifted(far2, -2), shifted(far1, -1)
    home, feature_parts = lax.optimization_barrier((home, feature_parts))
    layer_out = jnp.concatenate([feature_parts[j] for j in range(parts)], axis=1)
    total = (home + two.astype(F32) + one.astype(F32)).astype(BF)
    return layer_out, query_grad, total[:rows], total[rows:]


def solution(mesh):
    finer = Mesh(mesh.devices.reshape(8, 2, 4, 4, 2), ("z_far", "z_pair", "x", "y", "core"))
    token = P(DP, HEAD)

    return jax.shard_map(
        on_device,
        mesh=finer,
        in_specs=(token, token, token, token, P((*HEAD, *DP), None), P()),
        out_specs=(token,) * 4,
        check_vma=False,
    )
```

```python
import functools
import math

import jax
import jax.numpy as jnp
from jax import lax
from jax.experimental import pallas as pl
from jax.experimental.pallas import tpu as pltpu
from jax.sharding import Mesh
from jax.sharding import PartitionSpec as P

HD = 128
LOG2E = 1.4426950408889634
NT = (((1,), (1,)), ((), ()))
HEAD = ("y", "core")
DP = ("z_far", "z_pair", "x")
BF = jnp.bfloat16
F32 = jnp.float32
HEADS = 8


def dot_nt(a, b):
    return lax.dot_general(a, b, NT, preferred_element_type=F32)


def dot_nn(a, b):
    return jnp.dot(a, b, preferred_element_type=F32)


def call(body, flops, **spec):
    return pl.pallas_call(
        body,
        compiler_params=pltpu.CompilerParams(dimension_semantics=("arbitrary",) * len(spec["grid"])),
        cost_estimate=pl.CostEstimate(flops=flops, transcendentals=0, bytes_accessed=8 << 20),
        **spec,
    )


def forward_body(scaling, group, lengths, place, q, k2, k1, k0, v2, v1, v0, att, shares, bias, vt):
    rows = q.shape[0]
    blocks = 3

    @pl.when(pl.program_id(0) == 0)
    def _():
        first = place[0] * rows
        at = first + lax.broadcasted_iota(jnp.int32, (1, rows), 1)

        def doc(d, carry):
            end, start = carry
            end = end + lengths[d]
            return end, jnp.where(end <= at, end, start)

        _, start = lax.fori_loop(0, lengths.shape[0], doc, (jnp.int32(0), jnp.zeros((1, rows), jnp.int32)))
        keyed = first - (blocks - 1) * rows + lax.broadcasted_iota(jnp.int32, (blocks * rows, rows), 0)
        bias[...] = jnp.where((keyed >= start) & (keyed <= at), 0.0, -1e30)
        for j, v in enumerate((v2, v1, v0)):
            vt[:, j * rows : (j + 1) * rows] = v[...].T

    for h in range(group):
        cols = slice(h * HD, (h + 1) * HD)
        qh = q[:, cols]
        s = [
            dot_nt(k[...], qh) * (scaling * LOG2E) + bias[j * rows : (j + 1) * rows, :]
            for j, k in enumerate((k2, k1, k0))
        ]
        top = functools.reduce(jnp.maximum, [jnp.max(x, axis=0, keepdims=True) for x in s])
        e = [jnp.exp2(x - top) for x in s]
        inv = 1.0 / sum(jnp.sum(x, axis=0, keepdims=True) for x in e)
        out = jnp.zeros((HD, rows), F32)
        for j, x in enumerate(e):
            p = (x * inv).astype(BF)
            shares[h, j * rows : (j + 1) * rows, :] = p
            out = out + dot_nn(vt[:, j * rows : (j + 1) * rows], p)
        att[:, cols] = out.T.astype(BF)


def pair_specs(rows):
    key, value = pl.BlockSpec((rows, HD), lambda i: (0, 0)), pl.BlockSpec((rows, HD), lambda i: (1, 0))
    return [key] * 3 + [value] * 3


def forward(lengths, place, q, pairs, group=2):
    rows, width = q.shape
    heads = width // HD
    smem = pl.BlockSpec(memory_space=pltpu.SMEM)
    return call(
        functools.partial(forward_body, 1.0 / math.sqrt(HD), group),
        8 << 30,
        grid=(heads // group,),
        in_specs=[smem, smem, pl.BlockSpec((rows, group * HD), lambda i: (0, i))] + pair_specs(rows),
        out_specs=[
            pl.BlockSpec((rows, group * HD), lambda i: (0, i)),
            pl.BlockSpec((group, 3 * rows, rows), lambda i: (i, 0, 0)),
        ],
        out_shape=[
            jax.ShapeDtypeStruct((rows, width), BF),
            jax.ShapeDtypeStruct((heads, 3 * rows, rows), BF),
        ],
        scratch_shapes=[pltpu.VMEM((3 * rows, rows), F32), pltpu.VMEM((HD, 3 * rows), BF)],
    )(lengths, place, q, *pairs, *pairs)


def backward_body(scaling, group, q, k2, k1, k0, v2, v1, v0, d_parts, att, shares, dq, far2, far1, home, kt, dka, dva):
    rows = q.shape[0]
    step = pl.program_id(0)

    @pl.when(step == 0)
    def _():
        for j, k in enumerate((k2, k1, k0)):
            kt[:, j * rows : (j + 1) * rows] = k[...].T
        dka[...] = jnp.zeros_like(dka)
        dva[...] = jnp.zeros_like(dva)

    spans = [slice(h * HD, (h + 1) * HD) for h in range(group)]
    das = [sum(d_parts[i, :, cols].astype(F32) for i in range(d_parts.shape[0])).astype(BF) for cols in spans]
    prods = [da.astype(F32) * att[:, cols].astype(F32) for da, cols in zip(das, spans)]
    dots = [jnp.sum(prod.T, axis=0, keepdims=True) for prod in prods]
    stacked_q = jnp.concatenate([q[:, cols] for cols in spans], axis=0)
    stacked_da = jnp.concatenate(das, axis=0)
    outs = [jnp.zeros((HD, rows), F32)] * group
    for j, v in enumerate((v2, v1, v0)):
        own = slice(j * rows, (j + 1) * rows)
        low = [shares[h, own, :] for h in range(group)]
        ds = [(p.astype(F32) * (dot_nt(v[...], da) - dot)).astype(BF) for p, da, dot in zip(low, das, dots)]
        outs = [out + dot_nn(kt[:, own], d) for out, d in zip(outs, ds)]
        dka[own, :] += dot_nn(jnp.concatenate(ds, axis=1), stacked_q)
        dva[own, :] += dot_nn(jnp.concatenate(low, axis=1), stacked_da)
    for cols, out in zip(spans, outs):
        dq[:, cols] = (out.T * scaling).astype(BF)

    @pl.when(step == pl.num_programs(0) - 1)
    def _():
        for j, to in enumerate((far2, far1, home)):
            own = slice(j * rows, (j + 1) * rows)
            to[:rows, :] = (dka[own, :] * scaling).astype(to.dtype)
            to[rows:, :] = dva[own, :].astype(to.dtype)


def backward(q, pairs, d_parts, att, shares, group=4):
    rows, width = q.shape
    heads = width // HD
    head = pl.BlockSpec((rows, group * HD), lambda i: (0, i))
    pair = pl.BlockSpec((2 * rows, HD), lambda i: (0, 0))
    return call(
        functools.partial(backward_body, 1.0 / math.sqrt(HD), group),
        8 << 30,
        grid=(heads // group,),
        in_specs=[head]
        + pair_specs(rows)
        + [pl.BlockSpec((d_parts.shape[0], rows, group * HD), lambda i: (0, 0, i)), head]
        + [pl.BlockSpec((group, 3 * rows, rows), lambda i: (i, 0, 0))],
        out_specs=[head] + [pair] * 3,
        out_shape=[jax.ShapeDtypeStruct((rows, width), BF)]
        + [jax.ShapeDtypeStruct((2 * rows, HD), t) for t in (BF, BF, F32)],
        scratch_shapes=[
            pltpu.VMEM((HD, 3 * rows), BF),
            pltpu.VMEM((3 * rows, HD), F32),
            pltpu.VMEM((3 * rows, HD), F32),
        ],
    )(q, *pairs, *pairs, d_parts, att, shares)


def back_body(og, w, out, lhs):
    @pl.when(pl.program_id(0) == 0)
    def _():
        for h in range(og.shape[0]):
            lhs[:, h * HD : (h + 1) * HD] = og[h]

    rows = out.shape[1]
    done = dot_nt(lhs[...], w[...]).astype(BF)
    for b in range(out.shape[0]):
        out[b] = done[b * rows : (b + 1) * rows]


def project_back(og, w, parts, block=256):
    _, tokens, _ = og.shape
    inner, columns = w.shape
    rows = tokens // parts
    return call(
        back_body,
        2 << 30,
        grid=(inner // block,),
        in_specs=[pl.BlockSpec(memory_space=pltpu.VMEM), pl.BlockSpec((block, columns), lambda i: (i, 0))],
        out_specs=pl.BlockSpec((parts, rows, block), lambda i: (0, 0, i)),
        out_shape=jax.ShapeDtypeStruct((parts, rows, inner), BF),
        scratch_shapes=[pltpu.VMEM((tokens, columns), BF)],
    )(og, w)


def out_body(parts, index, side, *refs):
    blocks, w0, w1, add = refs[:parts], refs[parts], refs[parts + 1], refs[parts + 3 : -2]
    out, lhs = refs[-2:]
    rows = blocks[0].shape[0]

    @pl.when(pl.program_id(0) == 0)
    def _():
        for k, block in enumerate(blocks):
            owner = lax.rem(index[0] + parts - k, parts)
            lhs[pl.ds(pl.multiple_of(owner * rows, rows), rows), :] = block[...]

    done = dot_nn(lhs[...], jnp.concatenate([w0[...], w1[...]], axis=1))
    for n in range(2):
        value = done[:, n * HD : (n + 1) * HD]
        for more in add:
            value = value + more[2 * pl.program_id(0) + n].astype(F32)
        out[n] = value.astype(BF)


def project_out(index, side, blocks, w, after, *add):
    rows, inner = blocks[0].shape
    parts = len(blocks)
    whole = pl.BlockSpec(memory_space=pltpu.VMEM)
    part = pl.BlockSpec((2, parts * rows, HD), lambda i, x, s: (i, 0, 0))
    columns = [pl.BlockSpec((inner, HD), lambda i, x, s, n=n: (0, 4 * i + 2 * n + s[0])) for n in range(2)]
    return pl.pallas_call(
        functools.partial(out_body, parts),
        grid_spec=pltpu.PrefetchScalarGridSpec(
            num_scalar_prefetch=2,
            grid=(HEADS // 4,),
            in_specs=[whole] * parts + columns + [pl.BlockSpec(memory_space=pl.ANY)] + [whole] * len(add),
            out_specs=part,
            scratch_shapes=[pltpu.VMEM((parts * rows, inner), BF)],
        ),
        out_shape=jax.ShapeDtypeStruct((HEADS // 2, parts * rows, HD), BF),
        compiler_params=pltpu.CompilerParams(dimension_semantics=("arbitrary",)),
        cost_estimate=pl.CostEstimate(flops=1 << 30, transcendentals=0, bytes_accessed=4 << 20),
        name="project_out",
    )(index, side, *blocks, w, w, after, *add)


def swap(pieces, axis):
    return lax.all_to_all(pieces, axis, 0, 0, tiled=True)


def everywhere(x, axis):
    return swap(jnp.broadcast_to(x[None], (lax.axis_size(axis), *x.shape)), axis)


def shifted(block, distance):
    size = lax.axis_size(DP)
    return lax.ppermute(block, DP, [(i, i + distance) for i in range(size) if 0 <= i + distance < size])


def partner(block, axis):
    return lax.ppermute(block, axis, [(i, i ^ 1) for i in range(lax.axis_size(axis))])


def around(blocks, axis, step):
    size = lax.axis_size(axis)
    return [blocks[0]] + [
        lax.ppermute(blocks[k], axis, [(i, (i + k * step) % size) for i in range(size)]) for k in range(1, size)
    ]


def on_device(queries, keys, values, output_grad, out_weight, lengths):
    rows = queries.shape[0]
    few = out_weight.shape[0]
    parts = lax.axis_size("x")
    place = lax.axis_index(DP).astype(jnp.int32).reshape(1)
    index = lax.axis_index("x").astype(jnp.int32).reshape(1)
    core = lax.axis_index("core").astype(jnp.int32).reshape(1)
    own_w = out_weight.reshape(few, HEADS, parts, HD).transpose(2, 0, 1, 3).reshape(parts, few, HEADS * HD)
    own_w = jnp.concatenate([own_w] * 2, axis=0)
    own_w = swap(own_w, ("z_pair", "x")).reshape(-1, HEADS * HD)
    weight = lax.all_gather(own_w, "z_far", axis=0, tiled=True)
    pair = jnp.concatenate([keys, values], axis=0)
    pairs = [shifted(pair, 2), shifted(pair, 1), pair]
    own_g = output_grad.reshape(rows, parts, HD).transpose(1, 0, 2)
    grads = swap(own_g, "x").reshape(parts * rows, HD)
    grads = everywhere(grads, HEAD)
    attended, shares = forward(lengths, place, queries, pairs)
    attended_all = around([attended] * parts, "x", 1)

    d_here = project_back(grads, weight, parts)
    d_parts = swap(d_here, "x")
    outward = project_out(index, 1 - core, attended_all, weight, d_here)
    outward = partner(outward, "core")
    projected = project_out(index, core, attended_all, weight, d_here, outward)
    projected = swap(projected.reshape(-1, rows, HD), ("y", "x"))
    feature_parts = projected.reshape(-1, parts, rows, HD).astype(F32).sum(axis=0).astype(BF)
    query_grad, far2, far1, home = backward(queries, pairs, d_parts, attended, shares)
    two, one = shifted(far2, -2), shifted(far1, -1)
    home, feature_parts = lax.optimization_barrier((home, feature_parts))
    layer_out = jnp.concatenate([feature_parts[j] for j in range(parts)], axis=1)
    total = (home + two.astype(F32) + one.astype(F32)).astype(BF)
    return layer_out, query_grad, total[:rows], total[rows:]


def solution(mesh):
    finer = Mesh(mesh.devices.reshape(8, 2, 4, 4, 2), ("z_far", "z_pair", "x", "y", "core"))
    token = P(DP, HEAD)

    return jax.shard_map(
        on_device,
        mesh=finer,
        in_specs=(token, token, token, token, P((*HEAD, *DP), None), P()),
        out_specs=(token,) * 4,
        check_vma=False,
    )
```

```python
import functools
import math

import jax
import jax.numpy as jnp
from jax import lax
from jax.experimental import pallas as pl
from jax.experimental.pallas import tpu as pltpu
from jax.sharding import Mesh
from jax.sharding import PartitionSpec as P

HD = 128
LOG2E = 1.4426950408889634
NT = (((1,), (1,)), ((), ()))
HEAD = ("y", "core")
DP = ("z_far", "z_pair", "x")
BF = jnp.bfloat16
F32 = jnp.float32
HEADS = 8


def dot_nt(a, b):
    return lax.dot_general(a, b, NT, preferred_element_type=F32)


def dot_nn(a, b):
    return jnp.dot(a, b, preferred_element_type=F32)


def call(body, flops, **spec):
    return pl.pallas_call(
        body,
        compiler_params=pltpu.CompilerParams(dimension_semantics=("arbitrary",) * len(spec["grid"])),
        cost_estimate=pl.CostEstimate(flops=flops, transcendentals=0, bytes_accessed=8 << 20),
        **spec,
    )


def forward_body(scaling, group, lengths, place, q, k2, k1, k0, v2, v1, v0, att, shares, bias, vt):
    rows = q.shape[0]
    blocks = 3

    @pl.when(pl.program_id(0) == 0)
    def _():
        first = place[0] * rows
        at = first + lax.broadcasted_iota(jnp.int32, (1, rows), 1)

        def doc(d, carry):
            end, start = carry
            end = end + lengths[d]
            return end, jnp.where(end <= at, end, start)

        _, start = lax.fori_loop(0, lengths.shape[0], doc, (jnp.int32(0), jnp.zeros((1, rows), jnp.int32)))
        keyed = first - (blocks - 1) * rows + lax.broadcasted_iota(jnp.int32, (blocks * rows, rows), 0)
        bias[...] = jnp.where((keyed >= start) & (keyed <= at), 0.0, -1e30)
        for j, v in enumerate((v2, v1, v0)):
            vt[:, j * rows : (j + 1) * rows] = v[...].T

    for h in range(group):
        cols = slice(h * HD, (h + 1) * HD)
        qh = q[:, cols]
        s = [
            dot_nt(k[...], qh) * (scaling * LOG2E) + bias[j * rows : (j + 1) * rows, :]
            for j, k in enumerate((k2, k1, k0))
        ]
        top = functools.reduce(jnp.maximum, [jnp.max(x, axis=0, keepdims=True) for x in s])
        e = [jnp.exp2(x - top) for x in s]
        inv = 1.0 / sum(jnp.sum(x, axis=0, keepdims=True) for x in e)
        out = jnp.zeros((HD, rows), F32)
        for j, x in enumerate(e):
            p = (x * inv).astype(BF)
            shares[h, j * rows : (j + 1) * rows, :] = p
            out = out + dot_nn(vt[:, j * rows : (j + 1) * rows], p)
        att[:, cols] = out.T.astype(BF)


def pair_specs(rows):
    key, value = pl.BlockSpec((rows, HD), lambda i: (0, 0)), pl.BlockSpec((rows, HD), lambda i: (1, 0))
    return [key] * 3 + [value] * 3


def forward(lengths, place, q, pairs, group=2):
    rows, width = q.shape
    heads = width // HD
    smem = pl.BlockSpec(memory_space=pltpu.SMEM)
    return call(
        functools.partial(forward_body, 1.0 / math.sqrt(HD), group),
        8 << 30,
        grid=(heads // group,),
        in_specs=[smem, smem, pl.BlockSpec((rows, group * HD), lambda i: (0, i))] + pair_specs(rows),
        out_specs=[
            pl.BlockSpec((rows, group * HD), lambda i: (0, i)),
            pl.BlockSpec((group, 3 * rows, rows), lambda i: (i, 0, 0)),
        ],
        out_shape=[
            jax.ShapeDtypeStruct((rows, width), BF),
            jax.ShapeDtypeStruct((heads, 3 * rows, rows), BF),
        ],
        scratch_shapes=[pltpu.VMEM((3 * rows, rows), F32), pltpu.VMEM((HD, 3 * rows), BF)],
    )(lengths, place, q, *pairs, *pairs)


def backward_body(scaling, group, q, k2, k1, k0, v2, v1, v0, d_parts, att, shares, dq, far2, far1, home, kt, dka, dva):
    rows = q.shape[0]
    step = pl.program_id(0)

    @pl.when(step == 0)
    def _():
        for j, k in enumerate((k2, k1, k0)):
            kt[:, j * rows : (j + 1) * rows] = k[...].T
        dka[...] = jnp.zeros_like(dka)
        dva[...] = jnp.zeros_like(dva)

    spans = [slice(h * HD, (h + 1) * HD) for h in range(group)]
    das = [sum(d_parts[i, :, cols].astype(F32) for i in range(d_parts.shape[0])).astype(BF) for cols in spans]
    prods = [da.astype(F32) * att[:, cols].astype(F32) for da, cols in zip(das, spans)]
    dots = [jnp.sum(prod.T, axis=0, keepdims=True) for prod in prods]
    stacked_q = jnp.concatenate([q[:, cols] for cols in spans], axis=0)
    stacked_da = jnp.concatenate(das, axis=0)
    outs = [jnp.zeros((HD, rows), F32)] * group
    for j, v in enumerate((v2, v1, v0)):
        own = slice(j * rows, (j + 1) * rows)
        low = [shares[h, own, :] for h in range(group)]
        ds = [(p.astype(F32) * (dot_nt(v[...], da) - dot)).astype(BF) for p, da, dot in zip(low, das, dots)]
        outs = [out + dot_nn(kt[:, own], d) for out, d in zip(outs, ds)]
        dka[own, :] += dot_nn(jnp.concatenate(ds, axis=1), stacked_q)
        dva[own, :] += dot_nn(jnp.concatenate(low, axis=1), stacked_da)
    for cols, out in zip(spans, outs):
        dq[:, cols] = (out.T * scaling).astype(BF)

    @pl.when(step == pl.num_programs(0) - 1)
    def _():
        for j, to in enumerate((far2, far1, home)):
            own = slice(j * rows, (j + 1) * rows)
            to[:rows, :] = (dka[own, :] * scaling).astype(to.dtype)
            to[rows:, :] = dva[own, :].astype(to.dtype)


def backward(q, pairs, d_parts, att, shares, group=4):
    rows, width = q.shape
    heads = width // HD
    head = pl.BlockSpec((rows, group * HD), lambda i: (0, i))
    pair = pl.BlockSpec((2 * rows, HD), lambda i: (0, 0))
    return call(
        functools.partial(backward_body, 1.0 / math.sqrt(HD), group),
        8 << 30,
        grid=(heads // group,),
        in_specs=[head]
        + pair_specs(rows)
        + [pl.BlockSpec((d_parts.shape[0], rows, group * HD), lambda i: (0, 0, i)), head]
        + [pl.BlockSpec((group, 3 * rows, rows), lambda i: (i, 0, 0))],
        out_specs=[head] + [pair] * 3,
        out_shape=[jax.ShapeDtypeStruct((rows, width), BF)]
        + [jax.ShapeDtypeStruct((2 * rows, HD), t) for t in (BF, BF, F32)],
        scratch_shapes=[
            pltpu.VMEM((HD, 3 * rows), BF),
            pltpu.VMEM((3 * rows, HD), F32),
            pltpu.VMEM((3 * rows, HD), F32),
        ],
    )(q, *pairs, *pairs, d_parts, att, shares)


def back_body(cot, w, out):
    rows = out.shape[1]
    done = dot_nt(cot[...], w[...]).astype(BF)
    for b in range(out.shape[0]):
        out[b] = done[b * rows : (b + 1) * rows]


def project_back(cot, w, parts, block=256):
    tokens, columns = cot.shape
    inner = w.shape[0]
    rows = tokens // parts
    return call(
        back_body,
        2 << 30,
        grid=(inner // block,),
        in_specs=[pl.BlockSpec((tokens, columns), lambda i: (0, 0)), pl.BlockSpec((block, columns), lambda i: (i, 0))],
        out_specs=pl.BlockSpec((parts, rows, block), lambda i: (0, 0, i)),
        out_shape=jax.ShapeDtypeStruct((parts, rows, inner), BF),
    )(cot, w)


def out_body(parts, index, side, *refs):
    blocks, w0, w1, add = refs[:parts], refs[parts], refs[parts + 1], refs[parts + 3 : -2]
    out, lhs = refs[-2:]
    rows = blocks[0].shape[0]

    @pl.when(pl.program_id(0) == 0)
    def _():
        for k, block in enumerate(blocks):
            owner = lax.rem(index[0] + parts - k, parts)
            lhs[pl.ds(pl.multiple_of(owner * rows, rows), rows), :] = block[...]

    done = dot_nn(lhs[...], jnp.concatenate([w0[...], w1[...]], axis=1))
    for n in range(2):
        value = done[:, n * HD : (n + 1) * HD]
        for more in add:
            value = value + more[2 * pl.program_id(0) + n].astype(F32)
        out[n] = value.astype(BF)


def project_out(index, side, blocks, w, after, *add):
    rows, inner = blocks[0].shape
    parts = len(blocks)
    whole = pl.BlockSpec(memory_space=pltpu.VMEM)
    part = pl.BlockSpec((2, parts * rows, HD), lambda i, x, s: (i, 0, 0))
    columns = [pl.BlockSpec((inner, HD), lambda i, x, s, n=n: (0, 4 * i + 2 * n + s[0])) for n in range(2)]
    return pl.pallas_call(
        functools.partial(out_body, parts),
        grid_spec=pltpu.PrefetchScalarGridSpec(
            num_scalar_prefetch=2,
            grid=(HEADS // 4,),
            in_specs=[whole] * parts + columns + [pl.BlockSpec(memory_space=pl.ANY)] + [whole] * len(add),
            out_specs=part,
            scratch_shapes=[pltpu.VMEM((parts * rows, inner), BF)],
        ),
        out_shape=jax.ShapeDtypeStruct((HEADS // 2, parts * rows, HD), BF),
        compiler_params=pltpu.CompilerParams(dimension_semantics=("arbitrary",)),
        cost_estimate=pl.CostEstimate(flops=1 << 30, transcendentals=0, bytes_accessed=4 << 20),
        name="project_out",
    )(index, side, *blocks, w, w, after, *add)


def swap(pieces, axis):
    return lax.all_to_all(pieces, axis, 0, 0, tiled=True)


def everywhere(x, axis):
    return swap(jnp.broadcast_to(x[None], (lax.axis_size(axis), *x.shape)), axis)


def shifted(block, distance):
    size = lax.axis_size(DP)
    return lax.ppermute(block, DP, [(i, i + distance) for i in range(size) if 0 <= i + distance < size])


def partner(block, axis):
    return lax.ppermute(block, axis, [(i, i ^ 1) for i in range(lax.axis_size(axis))])


def around(blocks, axis, step):
    size = lax.axis_size(axis)
    return [blocks[0]] + [
        lax.ppermute(blocks[k], axis, [(i, (i + k * step) % size) for i in range(size)]) for k in range(1, size)
    ]


def on_device(queries, keys, values, output_grad, out_weight, lengths):
    rows = queries.shape[0]
    few = out_weight.shape[0]
    parts = lax.axis_size("x")
    place = lax.axis_index(DP).astype(jnp.int32).reshape(1)
    index = lax.axis_index("x").astype(jnp.int32).reshape(1)
    core = lax.axis_index("core").astype(jnp.int32).reshape(1)
    own_w = out_weight.reshape(few, HEADS, parts, HD).transpose(2, 0, 1, 3).reshape(parts, few, HEADS * HD)
    own_w = jnp.concatenate([own_w] * 2, axis=0)
    own_w = swap(own_w, ("z_pair", "x")).reshape(-1, HEADS * HD)
    weight = lax.all_gather(own_w, "z_far", axis=0, tiled=True)
    pair = jnp.concatenate([keys, values], axis=0)
    pairs = [shifted(pair, 2), shifted(pair, 1), pair]
    own_g = output_grad.reshape(rows, parts, HD).transpose(1, 0, 2)
    grads = swap(own_g, "x").reshape(parts * rows, HD)
    grads = everywhere(grads, HEAD).transpose(1, 0, 2).reshape(parts * rows, HEADS * HD)
    attended, shares = forward(lengths, place, queries, pairs)
    attended_all = around([attended] * parts, "x", 1)

    d_here = project_back(grads, weight, parts)
    d_parts = swap(d_here, "x")
    outward = project_out(index, 1 - core, attended_all, weight, d_here)
    outward = partner(outward, "core")
    projected = project_out(index, core, attended_all, weight, d_here, outward)
    projected = swap(projected.reshape(-1, rows, HD), ("y", "x"))
    feature_parts = projected.reshape(-1, parts, rows, HD).astype(F32).sum(axis=0).astype(BF)
    query_grad, far2, far1, home = backward(queries, pairs, d_parts, attended, shares)
    two, one = shifted(far2, -2), shifted(far1, -1)
    layer_out = jnp.concatenate([feature_parts[j] for j in range(parts)], axis=1)
    home, layer_out = lax.optimization_barrier((home, layer_out))
    key_grad, value_grad = [
        (home[at] + two[at].astype(F32) + one[at].astype(F32)).astype(BF) for at in (slice(0, rows), slice(rows, None))
    ]
    return layer_out, query_grad, key_grad, value_grad


def solution(mesh):
    finer = Mesh(mesh.devices.reshape(8, 2, 4, 4, 2), ("z_far", "z_pair", "x", "y", "core"))
    token = P(DP, HEAD)

    return jax.shard_map(
        on_device,
        mesh=finer,
        in_specs=(token, token, token, token, P((*HEAD, *DP), None), P()),
        out_specs=(token,) * 4,
        check_vma=False,
    )
```

```python
import functools
import math

import jax
import jax.numpy as jnp
from jax import lax
from jax.experimental import pallas as pl
from jax.experimental.pallas import tpu as pltpu
from jax.sharding import Mesh
from jax.sharding import PartitionSpec as P

HD = 128
LOG2E = 1.4426950408889634
NT = (((1,), (1,)), ((), ()))
HEAD = ("y", "core")
DP = ("z_pair", "z_far", "x")
BF = jnp.bfloat16
F32 = jnp.float32
HEADS = 8


def dot_nt(a, b):
    return lax.dot_general(a, b, NT, preferred_element_type=F32)


def dot_nn(a, b):
    return jnp.dot(a, b, preferred_element_type=F32)


def call(body, flops, **spec):
    return pl.pallas_call(
        body,
        compiler_params=pltpu.CompilerParams(dimension_semantics=("arbitrary",) * len(spec["grid"])),
        cost_estimate=pl.CostEstimate(flops=flops, transcendentals=0, bytes_accessed=8 << 20),
        **spec,
    )


def forward_body(scaling, group, lengths, place, q, k2, k1, k0, v2, v1, v0, att, shares, bias, vt):
    rows = q.shape[0]
    blocks = 3

    @pl.when(pl.program_id(0) == 0)
    def _():
        first = place[0] * rows
        at = first + lax.broadcasted_iota(jnp.int32, (1, rows), 1)

        def doc(d, carry):
            end, start = carry
            end = end + lengths[d]
            return end, jnp.where(end <= at, end, start)

        _, start = lax.fori_loop(0, lengths.shape[0], doc, (jnp.int32(0), jnp.zeros((1, rows), jnp.int32)))
        keyed = first - (blocks - 1) * rows + lax.broadcasted_iota(jnp.int32, (blocks * rows, rows), 0)
        bias[...] = jnp.where((keyed >= start) & (keyed <= at), 0.0, -1e30)
        for j, v in enumerate((v2, v1, v0)):
            vt[:, j * rows : (j + 1) * rows] = v[...].T

    for h in range(group):
        cols = slice(h * HD, (h + 1) * HD)
        qh = q[:, cols]
        s = [
            dot_nt(k[...], qh) * (scaling * LOG2E) + bias[j * rows : (j + 1) * rows, :]
            for j, k in enumerate((k2, k1, k0))
        ]
        top = functools.reduce(jnp.maximum, [jnp.max(x, axis=0, keepdims=True) for x in s])
        e = [jnp.exp2(x - top) for x in s]
        inv = 1.0 / sum(jnp.sum(x, axis=0, keepdims=True) for x in e)
        out = jnp.zeros((HD, rows), F32)
        for j, x in enumerate(e):
            p = (x * inv).astype(BF)
            shares[h, j * rows : (j + 1) * rows, :] = p
            out = out + dot_nn(vt[:, j * rows : (j + 1) * rows], p)
        att[:, cols] = out.T.astype(BF)


def pair_specs(rows):
    key, value = pl.BlockSpec((rows, HD), lambda i: (0, 0)), pl.BlockSpec((rows, HD), lambda i: (1, 0))
    return [key] * 3 + [value] * 3


def forward(lengths, place, q, pairs, group=2):
    rows, width = q.shape
    heads = width // HD
    smem = pl.BlockSpec(memory_space=pltpu.SMEM)
    return call(
        functools.partial(forward_body, 1.0 / math.sqrt(HD), group),
        8 << 30,
        grid=(heads // group,),
        in_specs=[smem, smem, pl.BlockSpec((rows, group * HD), lambda i: (0, i))] + pair_specs(rows),
        out_specs=[
            pl.BlockSpec((rows, group * HD), lambda i: (0, i)),
            pl.BlockSpec((group, 3 * rows, rows), lambda i: (i, 0, 0)),
        ],
        out_shape=[
            jax.ShapeDtypeStruct((rows, width), BF),
            jax.ShapeDtypeStruct((heads, 3 * rows, rows), BF),
        ],
        scratch_shapes=[pltpu.VMEM((3 * rows, rows), F32), pltpu.VMEM((HD, 3 * rows), BF)],
    )(lengths, place, q, *pairs, *pairs)


def backward_body(scaling, group, q, k2, k1, k0, v2, v1, v0, d_parts, att, shares, dq, far2, far1, home, kt, dka, dva):
    rows = q.shape[0]
    step = pl.program_id(0)

    @pl.when(step == 0)
    def _():
        for j, k in enumerate((k2, k1, k0)):
            kt[:, j * rows : (j + 1) * rows] = k[...].T
        dka[...] = jnp.zeros_like(dka)
        dva[...] = jnp.zeros_like(dva)

    spans = [slice(h * HD, (h + 1) * HD) for h in range(group)]
    das = [sum(d_parts[i, :, cols].astype(F32) for i in range(d_parts.shape[0])).astype(BF) for cols in spans]
    prods = [da.astype(F32) * att[:, cols].astype(F32) for da, cols in zip(das, spans)]
    dots = [jnp.sum(prod.T, axis=0, keepdims=True) for prod in prods]
    stacked_q = jnp.concatenate([q[:, cols] for cols in spans], axis=0)
    stacked_da = jnp.concatenate(das, axis=0)
    outs = [jnp.zeros((HD, rows), F32)] * group
    for j, v in enumerate((v2, v1, v0)):
        own = slice(j * rows, (j + 1) * rows)
        low = [shares[h, own, :] for h in range(group)]
        ds = [(p.astype(F32) * (dot_nt(v[...], da) - dot)).astype(BF) for p, da, dot in zip(low, das, dots)]
        outs = [out + dot_nn(kt[:, own], d) for out, d in zip(outs, ds)]
        dka[own, :] += dot_nn(jnp.concatenate(ds, axis=1), stacked_q)
        dva[own, :] += dot_nn(jnp.concatenate(low, axis=1), stacked_da)
    for cols, out in zip(spans, outs):
        dq[:, cols] = (out.T * scaling).astype(BF)

    @pl.when(step == pl.num_programs(0) - 1)
    def _():
        for j, to in enumerate((far2, far1, home)):
            own = slice(j * rows, (j + 1) * rows)
            to[:rows, :] = (dka[own, :] * scaling).astype(to.dtype)
            to[rows:, :] = dva[own, :].astype(to.dtype)


def backward(q, pairs, d_parts, att, shares, group=4):
    rows, width = q.shape
    heads = width // HD
    head = pl.BlockSpec((rows, group * HD), lambda i: (0, i))
    pair = pl.BlockSpec((2 * rows, HD), lambda i: (0, 0))
    return call(
        functools.partial(backward_body, 1.0 / math.sqrt(HD), group),
        8 << 30,
        grid=(heads // group,),
        in_specs=[head]
        + pair_specs(rows)
        + [pl.BlockSpec((d_parts.shape[0], rows, group * HD), lambda i: (0, 0, i)), head]
        + [pl.BlockSpec((group, 3 * rows, rows), lambda i: (i, 0, 0))],
        out_specs=[head] + [pair] * 3,
        out_shape=[jax.ShapeDtypeStruct((rows, width), BF)]
        + [jax.ShapeDtypeStruct((2 * rows, HD), t) for t in (BF, BF, F32)],
        scratch_shapes=[
            pltpu.VMEM((HD, 3 * rows), BF),
            pltpu.VMEM((3 * rows, HD), F32),
            pltpu.VMEM((3 * rows, HD), F32),
        ],
    )(q, *pairs, *pairs, d_parts, att, shares)


def back_body(cot, w, out):
    rows = out.shape[1]
    done = dot_nt(cot[...], w[:, 0].reshape(-1, w.shape[-1])).astype(BF)
    for b in range(out.shape[0]):
        out[b] = done[b * rows : (b + 1) * rows]


def project_back(cot, w, parts, block=256):
    tokens, columns = cot.shape
    far, pair, deep, _ = w.shape
    inner = far * pair * deep
    rows = tokens // parts
    count = block // deep
    return call(
        back_body,
        2 << 30,
        grid=(inner // block,),
        in_specs=[pl.BlockSpec((tokens, columns), lambda i: (0, 0)), pl.BlockSpec((count, 1, deep, columns), lambda i: (lax.rem(i, far // count), lax.div(i, far // count), 0, 0))],
        out_specs=pl.BlockSpec((parts, rows, block), lambda i: (0, 0, i)),
        out_shape=jax.ShapeDtypeStruct((parts, rows, inner), BF),
    )(cot, w)


def out_body(parts, index, side, *refs):
    blocks, w0, w1, add = refs[:parts], refs[parts], refs[parts + 1], refs[parts + 3 : -2]
    out, lhs = refs[-2:]
    rows = blocks[0].shape[0]

    @pl.when(pl.program_id(0) == 0)
    def _():
        for k, block in enumerate(blocks):
            owner = lax.rem(index[0] + parts - k, parts)
            lhs[pl.ds(pl.multiple_of(owner * rows, rows), rows), :] = block[...]

    by_z = [jnp.concatenate([w[:, b].reshape(-1, HD) for b in range(w.shape[1])], axis=0) for w in (w0, w1)]
    done = dot_nn(lhs[...], jnp.concatenate(by_z, axis=1))
    for n in range(2):
        value = done[:, n * HD : (n + 1) * HD]
        for more in add:
            value = value + more[2 * pl.program_id(0) + n].astype(F32)
        out[n] = value.astype(BF)


def project_out(index, side, blocks, w, after, *add):
    rows, inner = blocks[0].shape
    parts = len(blocks)
    whole = pl.BlockSpec(memory_space=pltpu.VMEM)
    part = pl.BlockSpec((2, parts * rows, HD), lambda i, x, s: (i, 0, 0))
    columns = [pl.BlockSpec((*w.shape[:3], HD), lambda i, x, s, n=n: (0, 0, 0, 4 * i + 2 * n + s[0])) for n in range(2)]
    return pl.pallas_call(
        functools.partial(out_body, parts),
        grid_spec=pltpu.PrefetchScalarGridSpec(
            num_scalar_prefetch=2,
            grid=(HEADS // 4,),
            in_specs=[whole] * parts + columns + [pl.BlockSpec(memory_space=pl.ANY)] + [whole] * len(add),
            out_specs=part,
            scratch_shapes=[pltpu.VMEM((parts * rows, inner), BF)],
        ),
        out_shape=jax.ShapeDtypeStruct((HEADS // 2, parts * rows, HD), BF),
        compiler_params=pltpu.CompilerParams(dimension_semantics=("arbitrary",)),
        cost_estimate=pl.CostEstimate(flops=1 << 30, transcendentals=0, bytes_accessed=4 << 20),
        name="project_out",
    )(index, side, *blocks, w, w, after, *add)


def swap(pieces, axis):
    return lax.all_to_all(pieces, axis, 0, 0, tiled=True)


def everywhere(x, axis):
    return swap(jnp.broadcast_to(x[None], (lax.axis_size(axis), *x.shape)), axis)


def shifted(block, distance):
    size = lax.axis_size(DP)
    return lax.ppermute(block, DP, [(i, i + distance) for i in range(size) if 0 <= i + distance < size])


def partner(block, axis):
    return lax.ppermute(block, axis, [(i, i ^ 1) for i in range(lax.axis_size(axis))])


def around(blocks, axis, step):
    size = lax.axis_size(axis)
    return [blocks[0]] + [
        lax.ppermute(blocks[k], axis, [(i, (i + k * step) % size) for i in range(size)]) for k in range(1, size)
    ]


def on_device(queries, keys, values, output_grad, out_weight, lengths):
    rows = queries.shape[0]
    few = out_weight.shape[0]
    parts = lax.axis_size("x")
    place = lax.axis_index(DP).astype(jnp.int32).reshape(1)
    index = lax.axis_index("x").astype(jnp.int32).reshape(1)
    core = lax.axis_index("core").astype(jnp.int32).reshape(1)
    own_w = out_weight.reshape(few, HEADS, parts, HD).transpose(2, 0, 1, 3).reshape(parts, few, HEADS * HD)
    own_w = jnp.concatenate([own_w] * 2, axis=0)
    own_w = swap(own_w, ("z_pair", "x")).reshape(-1, HEADS * HD)
    weight = lax.all_gather(own_w, "z_far", axis=0, tiled=True).reshape(-1, 2, parts * few, HEADS * HD)
    pair = jnp.concatenate([keys, values], axis=0)
    pairs = [shifted(pair, 2), shifted(pair, 1), pair]
    own_g = output_grad.reshape(rows, parts, HD).transpose(1, 0, 2)
    grads = swap(own_g, "x").reshape(parts * rows, HD)
    grads = everywhere(grads, HEAD).transpose(1, 0, 2).reshape(parts * rows, HEADS * HD)
    attended, shares = forward(lengths, place, queries, pairs)
    attended_all = around([attended] * parts, "x", 1)

    d_here = project_back(grads, weight, parts)
    d_parts = swap(d_here, "x")
    outward = project_out(index, 1 - core, attended_all, weight, d_here)
    outward = partner(outward, "core")
    projected = project_out(index, core, attended_all, weight, d_here, outward)
    projected = swap(projected.reshape(-1, rows, HD), ("y", "x"))
    feature_parts = projected.reshape(-1, parts, rows, HD).astype(F32).sum(axis=0).astype(BF)
    query_grad, far2, far1, home = backward(queries, pairs, d_parts, attended, shares)
    two, one = shifted(far2, -2), shifted(far1, -1)
    layer_out = jnp.concatenate([feature_parts[j] for j in range(parts)], axis=1)
    home, layer_out = lax.optimization_barrier((home, layer_out))
    key_grad, value_grad = [
        (home[at] + two[at].astype(F32) + one[at].astype(F32)).astype(BF) for at in (slice(0, rows), slice(rows, None))
    ]
    return layer_out, query_grad, key_grad, value_grad


def solution(mesh):
    finer = Mesh(mesh.devices.reshape(2, 8, 4, 4, 2), ("z_pair", "z_far", "x", "y", "core"))
    token = P(DP, HEAD)

    return jax.shard_map(
        on_device,
        mesh=finer,
        in_specs=(token, token, token, token, P((*HEAD, *DP), None), P()),
        out_specs=(token,) * 4,
        check_vma=False,
    )
```
